128 devices in a mesh: depth: 4 (over y), row: 4 (over x), col: 8 (over z, core).
Axes of the slice: x: 4, y: 4, z: 4, core: 2. Of those that a mesh axis runs over, the one named last changes fastest.
Arguments:
- alignment: bfloat16 [256, 512, 256], P('depth', ('row', 'col')), may hold values from -6 to 6
- norm_gain: float32 [256], replicated, may hold values from 0.25 to 1.75
- norm_shift: float32 [256], replicated, may hold values from -3 to 3
- proj_weight: bfloat16 [256, 64], replicated, may hold values from -0.375 to 0.375
- proj_bias: float32 [64], replicated, may hold values from -3 to 3
- out_weight: bfloat16 [1024, 128], replicated, may hold values from -0.1875 to 0.1875
- out_bias: float32 [128], replicated, may hold values from -3 to 3
- cotangent: bfloat16 [512, 512, 128], P('row', 'col', 'depth'), may hold values from -6 to 6
Outputs:
- pair_update: bfloat16 [512, 512, 128], P('row', 'col', 'depth')
- grad_alignment: bfloat16 [256, 512, 256], P('depth', ('row', 'col'))
- grad_proj_weight: float32 [256, 64], replicated
- grad_proj_bias: float32 [64], replicated
- grad_out_weight: float32 [1024, 128], replicated
- grad_out_bias: float32 [128], replicated
- grad_norm_gain: float32 [256], replicated
- grad_norm_shift: float32 [256], replicated
The draws below stay inside these ranges and needn't reach their ends.
All inputs are finite; a program needn't handle non-finite values.
Results may differ from the reference program's by a relative error of at most 0.009.
Values may be sent and summed in bfloat16 or wider, within the bound.
No kernel may reach another device: no remote copies, remote signals or barrier semaphores. Data moves between devices by JAX's collectives and lax.ppermute only.
A program may use at most 64 MiB of HBM per device.

```python
import jax
import jax.numpy as jnp
from jax import lax

CHANNELS = 256
HID = 32
PAIR = 128
S_DEV = 64
SEQS = 256
RES = 512


def level_of(stream_key, dims, pieces, smallest, largest):
    def one(dim, blocks):
        heights = jax.random.uniform(jax.random.fold_in(jax.random.fold_in(stream_key, 6), dim), (blocks,), jnp.float32, smallest / len(pieces), largest / len(pieces))
        return jnp.repeat(jnp.exp(heights), dims[dim] // blocks).reshape((-1,) + (1,) * (len(dims) - dim - 1))

    loudness = one(*pieces[0])
    for cut in pieces[1:]:
        loudness = loudness * one(*cut)
    return loudness


def scatter_about(stream_key, dims, deviation, reach, cuts=(), held_as=jnp.bfloat16):
    factor_of = level_of(stream_key, dims, cuts, -0.22, 0.18) if cuts else 1.0
    result = jax.random.normal(stream_key, dims, jnp.float32) * deviation * factor_of
    return jnp.minimum(jnp.maximum(result, -reach), reach).astype(held_as)


def setup_inputs(seed: int = 0) -> dict:
    streams_of = jax.random.split(jax.random.key(seed), 9)
    return {
        "alignment": scatter_about(streams_of[0], (SEQS, RES, CHANNELS), 1.0, 6.0, ((0, 4), (1, 32))),
        "norm_gain": jnp.clip(1.0 + 0.15 * jax.random.normal(streams_of[1], (CHANNELS,), jnp.float32), 0.25, 1.75),
        "norm_shift": scatter_about(streams_of[2], (CHANNELS,), 0.4, 3.0, (), jnp.float32),
        "proj_weight": scatter_about(streams_of[3], (CHANNELS, 2 * HID), CHANNELS ** -0.5, 0.375),
        "proj_bias": scatter_about(streams_of[4], (2 * HID,), 0.5, 3.0, (), jnp.float32),
        "out_weight": scatter_about(streams_of[5], (HID * HID, PAIR), (HID * HID) ** -0.5, 0.1875),
        "out_bias": scatter_about(streams_of[6], (PAIR,), 0.5, 3.0, (), jnp.float32),
        "cotangent": scatter_about(streams_of[7], (RES, RES, PAIR), 1.0, 6.0, ((0, 4), (1, 8), (2, 4))),
    }


EPSILON = 1e-05

def layer_norm(values, scales, biases):
    centre = values - lax.optimization_barrier(jnp.mean(values, axis=-1, keepdims=True))
    spread = lax.optimization_barrier(jnp.mean(centre * centre, axis=-1, keepdims=True))
    return centre * lax.rsqrt(spread + EPSILON) * scales + biases

def to_bf16(values):
    return lax.optimization_barrier(values.astype(jnp.bfloat16)).astype(jnp.float32)

def reference(alignment, norm_gain, norm_shift, proj_weight, proj_bias, out_weight, out_bias, cotangent):
    align_float = alignment.astype(jnp.float32)
    normed_float, pullback = jax.vjp(layer_norm, align_float, norm_gain, norm_shift)
    normed = normed_float.astype(jnp.bfloat16)
    flat_norm = normed.reshape(SEQS * RES, CHANNELS)
    sides = (jnp.dot(flat_norm, proj_weight, preferred_element_type=jnp.float32) + proj_bias).astype(jnp.bfloat16)
    sides = sides.reshape(SEQS, RES, 2 * HID)
    left_side = sides[:, :, :HID].astype(jnp.float32)
    right_side = sides[:, :, HID:].astype(jnp.float32)
    scaled = to_bf16(cotangent.astype(jnp.float32) / SEQS)
    w_cube = out_weight.astype(jnp.float32).reshape(HID, HID, PAIR)
    group_count = SEQS // S_DEV
    right_groups = right_side.reshape(group_count, S_DEV, RES, HID)
    block_rows = min(RES, 8)
    block_count = RES // block_rows

    def advance(running, row_start):
        grad_wout, grad_right = running
        left_block = lax.dynamic_slice_in_dim(left_side, row_start, block_rows, 1)
        scaled_block = lax.dynamic_slice_in_dim(scaled, row_start, block_rows, 0)
        left_groups = left_block.reshape(group_count, S_DEV, block_rows, HID)
        grad_outer = to_bf16(jnp.einsum('ijp,cep->ijce', scaled_block, w_cube))
        summed = jnp.zeros((block_rows, RES, PAIR), jnp.float32)
        for group in range(group_count):
            outer_prod = to_bf16(jnp.einsum('sic,sje->ijce', left_groups[group], right_groups[group]))
            summed = summed + to_bf16(jnp.einsum('ijce,cep->ijp', outer_prod, w_cube))
            grad_wout = grad_wout + jnp.einsum('ijce,ijp->cep', outer_prod, scaled_block)
        grad_left = jnp.einsum('ijce,sje->sic', grad_outer, right_side)
        grad_right = grad_right + jnp.einsum('ijce,sic->sje', grad_outer, left_block)
        pair_block = (summed / SEQS + out_bias).astype(jnp.bfloat16)
        return ((grad_wout, grad_right), (pair_block, grad_left))
    starts = jnp.arange(block_count, dtype=jnp.int32) * block_rows
    initial = (jnp.zeros((HID, HID, PAIR), jnp.float32), jnp.zeros((SEQS, RES, HID), jnp.float32))
    (grad_wout, grad_right), (pair_blocks, left_grads) = lax.scan(advance, initial, starts)
    pair_update = pair_blocks.reshape(RES, RES, PAIR)
    grad_left = jnp.transpose(left_grads, (1, 0, 2, 3)).reshape(SEQS, RES, HID)
    grad_sides = jnp.concatenate([grad_left, grad_right], axis=-1).astype(jnp.bfloat16)
    flat_grad = grad_sides.reshape(SEQS * RES, 2 * HID)
    grad_proj_weight = jnp.dot(flat_norm.T, flat_grad, preferred_element_type=jnp.float32)
    grad_proj_bias = lax.optimization_barrier(jnp.sum(flat_grad.astype(jnp.float32), axis=0))
    grad_normed = jnp.dot(flat_grad, proj_weight.T, preferred_element_type=jnp.float32).reshape(SEQS, RES, CHANNELS)
    grad_align, grad_gain, grad_shift = pullback(grad_normed)
    grad_out_bias = lax.optimization_barrier(jnp.sum(cotangent.astype(jnp.float32), axis=(0, 1)))
    return (pair_update, grad_align.astype(jnp.bfloat16), grad_proj_weight, grad_proj_bias, grad_wout.reshape(HID * HID, PAIR), grad_out_bias, grad_gain, grad_shift)
```

```python
import jax
import jax.numpy as jnp
from jax import lax
from jax.experimental import pallas as pl
from jax.experimental.pallas import tpu as pltpu
from jax.sharding import Mesh
from jax.sharding import PartitionSpec as P

EPSILON = 1e-05
F32 = jnp.float32
BF16 = jnp.bfloat16
NN = (((1,), (0,)), ((), ()))
NT = (((1,), (1,)), ((), ()))
TN = (((0,), (0,)), ((), ()))


def dot(a, b, dims):
    return lax.dot_general(a, b, dims, preferred_element_type=F32)


def vmem(count):
    return [pl.BlockSpec(memory_space=pltpu.VMEM)] * count


def column_of(row):
    size = row.shape[1]
    on = lax.broadcasted_iota(jnp.int32, (size, size), 0) == lax.broadcasted_iota(
        jnp.int32, (size, size), 1
    )
    return jnp.sum(jnp.where(on, row, 0.0), axis=1, keepdims=True)


def sides_kernel(x_ref, gain_ref, shift_ref, wt_ref, bias_ref, out_ref, normed_ref, rows, packed):
    seqs, own = 64, 16
    gain, shift = gain_ref[...], shift_ref[...]

    def block(k, _):
        x = x_ref[pl.ds(k * 128, 128), :].astype(F32)
        centre = x - jnp.mean(x, axis=-1, keepdims=True)
        spread = jnp.mean(centre * centre, axis=-1, keepdims=True)
        y = centre * lax.rsqrt(spread + EPSILON) * gain + shift
        rows[0, pl.ds(k * 128, 128), :] = y[:, :128]
        rows[1, pl.ds(k * 128, 128), :] = y[:, 128:]
        return 0

    lax.fori_loop(0, 8, block, 0)
    for i in range(own):
        part = jnp.concatenate(
            [rows[h, pl.ds(i, seqs, stride=own), :] for h in range(2)], axis=1
        )
        normed_ref[i * seqs : (i + 1) * seqs, :] = part.astype(BF16)
    sides = dot(wt_ref[...], normed_ref[...], NT) + column_of(bias_ref[...])
    for i in range(own):
        t = sides[:, i * seqs : (i + 1) * seqs]
        for side in range(2):
            lo = t[side * 32 : side * 32 + 16]
            hi = t[side * 32 + 16 : side * 32 + 32]
            packed[pl.ds(side * 256 + i, 16, stride=own), :] = jnp.concatenate([lo, hi], axis=1)
    out_ref[...] = packed[...].astype(BF16).reshape(2, 16, own, 128)


def sides_call(x, gain, shift, wt, bias):
    return pl.pallas_call(
        sides_kernel,
        out_shape=(
            jax.ShapeDtypeStruct((2, 16, 16, 128), BF16),
            jax.ShapeDtypeStruct((1024, 256), BF16),
        ),
        in_specs=vmem(5),
        out_specs=tuple(vmem(2)),
        scratch_shapes=[pltpu.VMEM((2, 1024, 128), F32), pltpu.VMEM((512, 128), F32)],
        cost_estimate=pl.CostEstimate(flops=60_000_000, bytes_accessed=1_200_000, transcendentals=1024),
        name="sides",
    )(x, gain, shift, wt, bias)


def left_kernel(
    r0_ref, r1_ref, r2_ref, r3_ref, s_ref, w_ref,
    keep_ref, send_ref, gp_ref, st_ref, rt_ref, gb_ref,
    tall, rbuf,
):
    core = lax.axis_index("col_1")
    row = lax.axis_index("row")
    for m, ref in enumerate((r0_ref, r1_ref, r2_ref, r3_ref)):
        rbuf[lax.rem(row + m, 4)] = ref[...].reshape(256, 128)
    for eh in range(2):
        for half in range(2):
            cut = [rbuf[2 * half + y][:, eh * 64 : eh * 64 + 64] for y in range(2)]
            rt_ref[eh * 256 : (eh + 1) * 256, half * 128 : (half + 1) * 128] = jnp.concatenate(
                cut, axis=1
            )
    for d in range(4):
        count = jnp.zeros((32, 128), F32)
        for j in range(16):
            t = s_ref[d, j].astype(F32)
            count = count + t
            st_ref[d * 32 : (d + 1) * 32, j * 128 : (j + 1) * 128] = (t * (1.0 / 256)).astype(
                BF16
            )
        gb_ref[d * 32 : (d + 1) * 32, :] = count

    for j in range(0, 16, 2):
        g = dot(w_ref[...], st_ref[:, j * 128 : (j + 2) * 128], NN)
        for jj in range(2):
            tall[:, (j + jj) * 8 : (j + jj + 1) * 8, :] = g[
                :, jj * 128 : (jj + 1) * 128
            ].reshape(128, 8, 128)

    def left(k, _):
        sums = []
        for ch in range(2):
            c = ch * 16 + k
            for e in range(32):
                gp_ref[c, e * 16 : (e + 1) * 16, :] = tall[
                    c * 4 + e // 8, pl.ds(e % 8, 16, stride=8), :
                ].astype(BF16)
            sums.append(dot(gp_ref[c], rt_ref[...], TN))
        for y in range(4):
            t = jnp.concatenate([v[:, y * 64 : (y + 1) * 64] for v in sums], axis=1)
            for z in range(4):
                a = t[z * 32 : z * 32 + 16]
                b = t[z * 32 + 16 : z * 32 + 32]
                keep_ref[z, y, k] = jnp.where(core == 0, a, b).astype(BF16)
                send_ref[z, y, k] = jnp.where(core == 0, b, a).astype(BF16)
        return 0

    lax.fori_loop(0, 16, left, 0)


def left_call(rs, s, w):
    return pl.pallas_call(
        left_kernel,
        out_shape=(
            jax.ShapeDtypeStruct((4, 4, 16, 16, 128), BF16),
            jax.ShapeDtypeStruct((4, 4, 16, 16, 128), BF16),
            jax.ShapeDtypeStruct((32, 512, 128), BF16),
            jax.ShapeDtypeStruct((128, 2048), BF16),
            jax.ShapeDtypeStruct((512, 256), BF16),
            jax.ShapeDtypeStruct((128, 128), F32),
        ),
        in_specs=vmem(6),
        out_specs=tuple(vmem(6)),
        scratch_shapes=[pltpu.VMEM((128, 128, 128), F32), pltpu.VMEM((4, 256, 128), BF16)],
        compiler_params=pltpu.CompilerParams(vmem_limit_bytes=24 * 2**20),
        cost_estimate=pl.CostEstimate(
            flops=6_000_000_000, bytes_accessed=8_000_000, transcendentals=0
        ),
        name="left",
    )(*rs, s, w)


def outer_kernel(
    near_ref, far_ref, rt_ref, st_ref, gp_ref, wt_ref,
    pair_ref, gr_ref, gw_ref,
    tall, xs, lt,
):
    core = lax.axis_index("col_1")
    row = lax.axis_index("row")

    def outer(k, _):
        for ref, side in ((near_ref, core), (far_ref, 1 - core)):
            for z in range(4):
                parts = [ref[z, y, k] for y in range(4)]
                for ch in range(2):
                    cut = [p[:, ch * 64 : ch * 64 + 64] for p in parts]
                    at = pl.multiple_of((ch * 16 + k) * 128 + (2 * z + side) * 16, 16)
                    lt[pl.ds(at, 16), 0:128] = jnp.concatenate(cut[:2], axis=1)
                    lt[pl.ds(at, 16), 128:256] = jnp.concatenate(cut[2:], axis=1)
        both = jnp.concatenate(
            [lt[pl.ds(pl.multiple_of((ch * 16 + k) * 128, 128), 128), :] for ch in range(2)],
            axis=0,
        )
        o = dot(rt_ref[...], both, NT)
        for ch in range(2):
            for e in range(32):
                tall[(ch * 16 + k) * 4 + e // 8, pl.ds(e % 8, 16, stride=8), :] = o[
                    e * 16 : (e + 1) * 16, ch * 128 : (ch + 1) * 128
                ]
        return 0

    lax.fori_loop(0, 16, outer, 0)

    wide = jnp.concatenate([gp_ref[c] for c in range(32)], axis=1)
    total = dot(wide, lt[...], NN)
    for y in range(4):
        t = jnp.concatenate(
            [total[eh * 256 : (eh + 1) * 256, y * 64 : (y + 1) * 64] for eh in range(2)], axis=1
        )
        gr_ref[lax.rem(y - row + 4, 4)] = t.astype(BF16).reshape(16, 16, 128)

    def convert(k, _):
        for j in range(16):
            xs[pl.ds(pl.multiple_of(k * 64, 64), 64), j * 128 : (j + 1) * 128] = (
                tall[pl.ds(k * 8, 8), j * 8 : (j + 1) * 8, :].reshape(64, 128).astype(BF16)
            )
        return 0

    lax.fori_loop(0, 16, convert, 0)

    for j in range(0, 16, 2):
        part = dot(wt_ref[...], xs[:, j * 128 : (j + 2) * 128], NN).astype(BF16)
        for jj in range(2):
            for d in range(4):
                pair_ref[d, j + jj] = part[d * 32 : (d + 1) * 32, jj * 128 : (jj + 1) * 128]

    def weight(k, _):
        at = pl.multiple_of(k * 256, 256)
        gw_ref[pl.ds(at, 256), :] = dot(xs[pl.ds(at, 256), :], st_ref[...], NT)
        return 0

    lax.fori_loop(0, 4, weight, 0)


def outer_call(near, far, rt, st, gp, wt):
    return pl.pallas_call(
        outer_kernel,
        out_shape=(
            jax.ShapeDtypeStruct((4, 16, 32, 128), BF16),
            jax.ShapeDtypeStruct((4, 16, 16, 128), BF16),
            jax.ShapeDtypeStruct((1024, 128), F32),
        ),
        in_specs=vmem(6),
        out_specs=tuple(vmem(3)),
        scratch_shapes=[
            pltpu.VMEM((128, 128, 128), F32),
            pltpu.VMEM((1024, 2048), BF16),
            pltpu.VMEM((4096, 256), BF16),
        ],
        compiler_params=pltpu.CompilerParams(vmem_limit_bytes=40 * 2**20),
        cost_estimate=pl.CostEstimate(
            flops=10_000_000_000, bytes_accessed=8_000_000, transcendentals=0
        ),
        name="outer",
    )(near, far, rt, st, gp, wt)


def back_kernel(
    x_ref, gain_ref, wt_ref, normed_ref, gl_ref, gr_ref,
    gx_ref, gw_ref, gb_ref, gg_ref, gs_ref,
    rows, sums, means, rstds,
):
    seqs, own = 64, 16
    gain = gain_ref[...]
    left = gl_ref[0].astype(F32)
    for k in range(1, gl_ref.shape[0]):
        left = left + gl_ref[k].astype(F32)
    right = gr_ref[0].astype(F32)
    for k in range(1, gr_ref.shape[0]):
        right = right + gr_ref[k].astype(F32)
    sums[0:256, :] = left.reshape(256, 128)
    sums[256:512, :] = right.reshape(256, 128)
    cuts = []
    for i in range(own):
        t = [sums[pl.ds(side * 256 + i, 16, stride=own), :] for side in range(2)]
        cuts.append(
            jnp.concatenate([t[0][:, :64], t[0][:, 64:], t[1][:, :64], t[1][:, 64:]], axis=0)
        )
    grad = jnp.concatenate(cuts, axis=1).astype(BF16)
    gb_ref[...] = jnp.sum(grad.astype(F32), axis=1, keepdims=True)
    gw_ref[...] = dot(grad, normed_ref[...], NN)

    def block(k, _):
        x = x_ref[pl.ds(k * 128, 128), :].astype(F32)
        mean = jnp.mean(x, axis=-1, keepdims=True)
        centre = x - mean
        spread = jnp.mean(centre * centre, axis=-1, keepdims=True)
        rstd = lax.rsqrt(spread + EPSILON)
        y = centre * rstd
        rows[0, pl.ds(k * 128, 128), :] = y[:, :128]
        rows[1, pl.ds(k * 128, 128), :] = y[:, 128:]
        rstds[pl.ds(k * 128, 128), :] = jnp.broadcast_to(rstd, (128, 128))
        return 0

    lax.fori_loop(0, 8, block, 0)
    gg = jnp.zeros((1, 256), F32)
    gs = jnp.zeros((1, 256), F32)
    for i in range(own):
        gn = dot(grad[:, i * seqs : (i + 1) * seqs], wt_ref[...], TN)
        hat = jnp.concatenate(
            [rows[h, pl.ds(i, seqs, stride=own), :] for h in range(2)], axis=1
        )
        rstd = rstds[pl.ds(i, seqs, stride=own), :][:, :1]
        gg = gg + jnp.sum(gn * hat, axis=0, keepdims=True)
        gs = gs + jnp.sum(gn, axis=0, keepdims=True)
        g = gn * gain
        a = jnp.mean(g, axis=-1, keepdims=True)
        b = jnp.mean(g * hat, axis=-1, keepdims=True)
        gx = rstd * (g - a - hat * b)
        for h in range(2):
            rows[h, pl.ds(i, seqs, stride=own), :] = gx[:, h * 128 : (h + 1) * 128]
    gg_ref[...] = gg
    gs_ref[...] = gs
    for h in range(2):
        gx_ref[:, h * 128 : (h + 1) * 128] = rows[h].astype(BF16)


def back_call(x, gain, wt, normed, gl, gr):
    return pl.pallas_call(
        back_kernel,
        out_shape=(
            jax.ShapeDtypeStruct((1024, 256), BF16),
            jax.ShapeDtypeStruct((64, 256), F32),
            jax.ShapeDtypeStruct((64, 1), F32),
            jax.ShapeDtypeStruct((1, 256), F32),
            jax.ShapeDtypeStruct((1, 256), F32),
        ),
        in_specs=vmem(6),
        out_specs=tuple(vmem(5)),
        scratch_shapes=[
            pltpu.VMEM((2, 1024, 128), F32),
            pltpu.VMEM((512, 128), F32),
            pltpu.VMEM((8, 128), F32),
            pltpu.VMEM((1024, 128), F32),
        ],
        cost_estimate=pl.CostEstimate(
            flops=120_000_000, bytes_accessed=2_000_000, transcendentals=1024
        ),
        name="back",
    )(x, gain, wt, normed, gl, gr)


def copies_of(value, axis):
    count = lax.axis_size(axis)
    return lax.all_to_all(
        jnp.broadcast_to(value[None], (count, *value.shape)), axis, 0, 0, tiled=True
    )


def exchange(value, axis):
    return lax.all_to_all(value, axis, 0, 0, tiled=True)


def swap(value):
    return lax.ppermute(value, "col_1", [(0, 1), (1, 0)])


def place(d, r, c):
    return (d * 4 + r) * 8 + c


def right_pairs():
    return [
        [
            (place(y, r, c), place(c % 4, (y - m) % 4, 2 * r + c // 4))
            for y in range(4)
            for r in range(4)
            for c in range(8)
        ]
        for m in range(4)
    ]


EVERY = ("depth", "row", "col_0", "col_1")
MANY = ("depth", "row", "col_0")


def summed(parts):
    return jnp.sum(parts.astype(F32), axis=0)


def on_device(
    alignment, norm_gain, norm_shift, proj_weight, proj_bias, out_weight, out_bias, cotangent
):
    x = alignment.reshape(1024, 256)
    gain = norm_gain.reshape(1, 256)
    shift = norm_shift.reshape(1, 256)
    wt = proj_weight.T
    cot = exchange(jnp.transpose(cotangent, (1, 2, 0)).reshape(4, 16, 32, 128), "depth")
    sides, normed = sides_call(x, gain, shift, wt, proj_bias.reshape(1, 64))
    pairs = right_pairs()
    rights = [lax.ppermute(sides[1], EVERY, p) for p in pairs]
    near = copies_of(copies_of(sides[0], "depth"), "col_0")
    far = swap(near)

    keep, send, gp, st, rt, count = left_call(rights, cot, out_weight)
    mine = keep.astype(F32) + swap(send).astype(F32)
    mine = summed(exchange(mine.astype(BF16), "col_0")).astype(BF16)
    lefts = exchange(mine, "depth")

    pair, gr, gw = outer_call(near, far, rt, st, gp, out_weight.T)
    back = [[(b, a) for a, b in p] for p in pairs]
    grads = jnp.stack([lax.ppermute(gr[m], EVERY, back[m]) for m in range(4)])

    pair = exchange(pair, "depth").reshape(64, 32, 128)
    depth = lax.axis_index("depth")
    bias = lax.dynamic_slice_in_dim(out_bias, depth * 32, 32, 0)
    pair_update = (pair.astype(F32) / 256 + bias[None, :, None]).astype(BF16)
    pair_update = jnp.transpose(pair_update, (2, 0, 1))

    core = lax.axis_index("col_1")
    halves = gw.reshape(2, 512, 128)
    kept = lax.dynamic_index_in_dim(halves, core, 0, keepdims=False)
    sent = lax.dynamic_index_in_dim(halves, 1 - core, 0, keepdims=False)
    half = (kept + swap(sent)).astype(BF16).reshape(64, 8, 128)
    half = summed(exchange(half, MANY)).astype(BF16)
    half = copies_of(half, MANY).reshape(512, 128)
    other = swap(half)
    gw_all = jnp.where(
        core == 0, jnp.concatenate([half, other]), jnp.concatenate([other, half])
    ).astype(F32)

    gx, gpw, gpb, gg, gs = back_call(x, gain, wt, normed, lefts, grads)
    flat = jnp.concatenate(
        [
            gpw.reshape(128, 128),
            jnp.sum(count, axis=1).reshape(1, 128),
            gg.reshape(2, 128),
            gs.reshape(2, 128),
            jnp.pad(gpb.reshape(1, 64), ((0, 0), (0, 64))),
            jnp.zeros((58, 128), F32),
        ]
    )
    flat = (flat + swap(flat)).reshape(64, 3, 128)
    flat = summed(exchange(flat, MANY))
    flat = copies_of(flat, MANY).reshape(192, 128)
    return (
        pair_update,
        gx.reshape(alignment.shape),
        flat[:128].reshape(64, 256).T,
        flat[133, :64],
        gw_all,
        flat[128],
        flat[129:131].reshape(256),
        flat[131:133].reshape(256),
    )


def solution(mesh):
    split = Mesh(mesh.devices.reshape(4, 4, 4, 2), EVERY)
    side = P("depth", ("row", "col_0", "col_1"), None)
    block = P("row", ("col_0", "col_1"), "depth")
    return jax.shard_map(
        on_device,
        mesh=split,
        in_specs=(side, P(), P(), P(), P(), P(), P(), block),
        out_specs=(block, side, P(), P(), P(), P(), P(), P()),
        check_vma=False,
    )
```

```python
import jax
import jax.numpy as jnp
from jax import lax
from jax.experimental import pallas as pl
from jax.experimental.pallas import tpu as pltpu
from jax.sharding import Mesh
from jax.sharding import PartitionSpec as P

EPSILON = 1e-05
F32 = jnp.float32
BF16 = jnp.bfloat16
NN = (((1,), (0,)), ((), ()))
NT = (((1,), (1,)), ((), ()))
TN = (((0,), (0,)), ((), ()))


def dot(a, b, dims):
    return lax.dot_general(a, b, dims, preferred_element_type=F32)


def vmem(count):
    return [pl.BlockSpec(memory_space=pltpu.VMEM)] * count


def hbm(count):
    return [pl.BlockSpec(memory_space=pltpu.HBM)] * count


def cost(us):
    return pl.CostEstimate(flops=us * 400_000_000, bytes_accessed=1_000_000, transcendentals=0)


def limit(mib):
    return pltpu.CompilerParams(vmem_limit_bytes=mib * 2**20)


def column_of(row):
    size = row.shape[1]
    on = lax.broadcasted_iota(jnp.int32, (size, size), 0) == lax.broadcasted_iota(
        jnp.int32, (size, size), 1
    )
    return jnp.sum(jnp.where(on, row, 0.0), axis=1, keepdims=True)


def sides_kernel(
    x_ref, gain_ref, shift_ref, wt_ref, bias_ref, left_ref, right_ref, normed_ref, rows, packed
):
    seqs, own = 64, 16
    gain, shift = gain_ref[...], shift_ref[...]

    def block(k, _):
        x = x_ref[pl.ds(k * 128, 128), :].astype(F32)
        centre = x - jnp.mean(x, axis=-1, keepdims=True)
        spread = jnp.mean(centre * centre, axis=-1, keepdims=True)
        hat = centre * lax.rsqrt(spread + EPSILON)
        rows[0, pl.ds(k * 128, 128), :] = hat[:, :128]
        rows[1, pl.ds(k * 128, 128), :] = hat[:, 128:]
        return 0

    lax.fori_loop(0, 8, block, 0)
    for i in range(own):
        hat = jnp.concatenate(
            [rows[h, pl.ds(i, seqs, stride=own), :] for h in range(2)], axis=1
        )
        at = slice(i * seqs, (i + 1) * seqs)
        normed_ref[at, :256] = (hat * gain + shift).astype(BF16)
        normed_ref[at, 256:] = hat.astype(BF16)
    sides = dot(wt_ref[...], normed_ref[:, :256], NT) + column_of(bias_ref[...])
    for i in range(own):
        t = sides[:, i * seqs : (i + 1) * seqs]
        for side in range(2):
            lo = t[side * 32 : side * 32 + 16]
            hi = t[side * 32 + 16 : side * 32 + 32]
            packed[pl.ds(side * 256 + i, 16, stride=own), :] = jnp.concatenate([lo, hi], axis=1)
    left = packed[:256, :].astype(BF16).reshape(16, own, 128)
    for peer in range(16):
        left_ref[peer] = left
    right_ref[...] = packed[256:, :].astype(BF16).reshape(16, own, 128)


def sides_call(x, gain, shift, wt, bias):
    return pl.pallas_call(
        sides_kernel,
        out_shape=(
            jax.ShapeDtypeStruct((16, 16, 16, 128), BF16),
            jax.ShapeDtypeStruct((16, 16, 128), BF16),
            jax.ShapeDtypeStruct((1024, 512), BF16),
        ),
        in_specs=vmem(5),
        out_specs=tuple(vmem(3)),
        scratch_shapes=[pltpu.VMEM((2, 1024, 128), F32), pltpu.VMEM((512, 128), F32)],
        cost_estimate=cost(4),
        name="sides",
    )(x, gain, shift, wt, bias)


def grad_kernel(s_ref, w_ref, gp_ref, st_ref, gb_ref, tall, held, sems):
    ones = lax.broadcasted_iota(jnp.int32, (128, 128), 0) == lax.broadcasted_iota(
        jnp.int32, (128, 128), 1
    )
    columns = []
    for d in range(4):
        count = jnp.zeros((32, 128), F32)
        for j in range(16):
            t = s_ref[d, j].astype(F32)
            count = count + t
            st_ref[d * 32 : (d + 1) * 32, j * 128 : (j + 1) * 128] = (t * (1.0 / 256)).astype(
                BF16
            )
        columns.append(jnp.sum(count, axis=1, keepdims=True))
    column = jnp.concatenate(columns, axis=0)
    gb_ref[...] = jnp.sum(jnp.where(ones, column, 0.0), axis=0, keepdims=True)

    for j in range(0, 16, 2):
        g = dot(w_ref[...], st_ref[:, j * 128 : (j + 2) * 128], NN)
        for jj in range(2):
            tall[:, (j + jj) * 8 : (j + jj + 1) * 8, :] = g[
                :, jj * 128 : (jj + 1) * 128
            ].reshape(128, 8, 128)

    def relay(c, _):
        for e in range(32):
            held[c, e * 16 : (e + 1) * 16, :] = tall[
                c * 4 + e // 8, pl.ds(e % 8, 16, stride=8), :
            ].astype(BF16)
        return 0

    copies = []
    for q in range(4):
        lax.fori_loop(q * 8, (q + 1) * 8, relay, 0)
        part = pl.ds(q * 8, 8)
        copies.append(pltpu.make_async_copy(held.at[part], gp_ref.at[part], sems.at[q]))
        copies[-1].start()
    for copy in copies:
        copy.wait()


def grad_call(s, w):
    return pl.pallas_call(
        grad_kernel,
        out_shape=(
            jax.ShapeDtypeStruct((32, 512, 128), BF16),
            jax.ShapeDtypeStruct((128, 2048), BF16),
            jax.ShapeDtypeStruct((1, 128), F32),
        ),
        in_specs=vmem(2),
        out_specs=(*hbm(1), *vmem(2)),
        scratch_shapes=[
            pltpu.VMEM((128, 128, 128), F32),
            pltpu.VMEM((32, 512, 128), BF16),
            pltpu.SemaphoreType.DMA((4,)),
        ],
        cost_estimate=cost(5),
        name="grad",
    )(s, w)


def left_kernel(
    r0_ref, r1_ref, r2_ref, r3_ref, gp_ref, keep_ref, send_ref, rt_ref,
    rbuf, held, sems, keep, send, out_sems,
):
    copies = []
    for q in range(8):
        part = pl.ds((q // 2 + q % 2 * 4) * 4, 4)
        copies.append(pltpu.make_async_copy(gp_ref.at[part], held.at[part], sems.at[q]))
        copies[-1].start()
    core = lax.axis_index("col_1")
    row = lax.axis_index("row")
    for m, ref in enumerate((r0_ref, r1_ref, r2_ref, r3_ref)):
        rbuf[lax.rem(row - m + 4, 4)] = ref[...].reshape(256, 128)
    for eh in range(2):
        for half in range(2):
            cut = [rbuf[2 * half + y][:, eh * 64 : eh * 64 + 64] for y in range(2)]
            rt_ref[eh * 256 : (eh + 1) * 256, half * 128 : (half + 1) * 128] = jnp.concatenate(
                cut, axis=1
            )

    def left(k, _):
        sums = [dot(held[ch * 16 + k], rt_ref[...], TN) for ch in range(2)]
        for y in range(4):
            t = jnp.concatenate([v[:, y * 64 : (y + 1) * 64] for v in sums], axis=1)
            for z in range(4):
                a = t[z * 32 : z * 32 + 16]
                b = t[z * 32 + 16 : z * 32 + 32]
                keep[y * 4 + z, k] = jnp.where(core == 0, a, b).astype(BF16)
                send[y * 4 + z, k] = jnp.where(core == 0, b, a).astype(BF16)
        return 0

    outs = []
    for q in range(4):
        copies[2 * q].wait()
        copies[2 * q + 1].wait()
        lax.fori_loop(q * 4, (q + 1) * 4, left, 0)
        part = pl.ds(q * 4, 4)
        outs.append(pltpu.make_async_copy(send.at[:, part], send_ref.at[:, part], out_sems.at[2 * q]))
        outs.append(pltpu.make_async_copy(keep.at[:, part], keep_ref.at[:, part], out_sems.at[2 * q + 1]))
        outs[-2].start()
        outs[-1].start()
    for copy in outs:
        copy.wait()


def left_call(rs, gp):
    return pl.pallas_call(
        left_kernel,
        out_shape=(
            jax.ShapeDtypeStruct((16, 16, 16, 128), BF16),
            jax.ShapeDtypeStruct((16, 16, 16, 128), BF16),
            jax.ShapeDtypeStruct((512, 256), BF16),
        ),
        in_specs=(*vmem(4), *hbm(1)),
        out_specs=(*hbm(2), *vmem(1)),
        scratch_shapes=[
            pltpu.VMEM((4, 256, 128), BF16),
            pltpu.VMEM((32, 512, 128), BF16),
            pltpu.SemaphoreType.DMA((8,)),
            pltpu.VMEM((16, 16, 16, 128), BF16),
            pltpu.VMEM((16, 16, 16, 128), BF16),
            pltpu.SemaphoreType.DMA((8,)),
        ],
        cost_estimate=cost(5),
        name="left",
    )(*rs, gp)


def right_kernel(
    near_ref, far_ref, gp_ref, g0_ref, g1_ref, g2_ref, g3_ref, lt_ref,
    gbuf, held, sems, near, far, lt,
):
    sides = [
        pltpu.make_async_copy(near_ref, near, sems.at[4]),
        pltpu.make_async_copy(far_ref, far, sems.at[5]),
    ]
    for copy in sides:
        copy.start()
    copies = []
    for q in range(4):
        part = pl.ds(q * 8, 8)
        copies.append(pltpu.make_async_copy(gp_ref.at[part], held.at[part], sems.at[q]))
        copies[-1].start()
    for copy in sides:
        copy.wait()
    core = lax.axis_index("col_1")
    row = lax.axis_index("row")

    def merge(k, _):
        for ref, side in ((near, core), (far, 1 - core)):
            for z in range(4):
                parts = [ref[y * 4 + z, k] for y in range(4)]
                for ch in range(2):
                    cut = [p[:, ch * 64 : ch * 64 + 64] for p in parts]
                    at = pl.multiple_of((ch * 16 + k) * 128 + (2 * z + side) * 16, 16)
                    lt[pl.ds(at, 16), 0:128] = jnp.concatenate(cut[:2], axis=1)
                    lt[pl.ds(at, 16), 128:256] = jnp.concatenate(cut[2:], axis=1)
        return 0

    lax.fori_loop(0, 16, merge, 0)
    kept = pltpu.make_async_copy(lt, lt_ref, sems.at[6])
    kept.start()

    for copy in copies:
        copy.wait()
    wide = jnp.concatenate([held[c] for c in range(32)], axis=1)
    total = dot(wide, lt[...], NN)
    for y in range(4):
        t = jnp.concatenate(
            [total[eh * 256 : (eh + 1) * 256, y * 64 : (y + 1) * 64] for eh in range(2)], axis=1
        )
        gbuf[y] = t.astype(BF16)
    for m, ref in enumerate((g0_ref, g1_ref, g2_ref, g3_ref)):
        ref[...] = gbuf[lax.rem(row + m, 4)].reshape(16, 16, 128)
    kept.wait()


def right_call(near, far, gp):
    return pl.pallas_call(
        right_kernel,
        out_shape=(
            *[jax.ShapeDtypeStruct((16, 16, 128), BF16)] * 4,
            jax.ShapeDtypeStruct((4096, 256), BF16),
        ),
        in_specs=hbm(3),
        out_specs=(*vmem(4), *hbm(1)),
        scratch_shapes=[
            pltpu.VMEM((4, 256, 128), BF16),
            pltpu.VMEM((32, 512, 128), BF16),
            pltpu.SemaphoreType.DMA((7,)),
            pltpu.VMEM((16, 16, 16, 128), BF16),
            pltpu.VMEM((16, 16, 16, 128), BF16),
            pltpu.VMEM((4096, 256), BF16),
        ],
        cost_estimate=cost(5),
        name="right",
    )(near, far, gp)


def outer_kernel(
    lt_ref, rt_ref, st_ref, w_ref, bias_ref, pair_ref, gw_ref, tall, xs, lt, sems
):
    copies = []
    for q in range(4):
        part = pl.ds(q * 1024, 1024)
        copies.append(pltpu.make_async_copy(lt_ref.at[part], lt.at[part], sems.at[q]))
        copies[-1].start()
    bias = column_of(bias_ref[...])

    def outer(k, _):
        both = lt[pl.ds(pl.multiple_of(k * 256, 256), 256), :]
        o = dot(rt_ref[...], both, NT)
        for ch in range(2):
            for e in range(32):
                tall[k * 8 + ch * 4 + e // 8, pl.ds(e % 8, 16, stride=8), :] = o[
                    e * 16 : (e + 1) * 16, ch * 128 : (ch + 1) * 128
                ]
        return 0

    for q in range(4):
        copies[q].wait()
        lax.fori_loop(q * 4, (q + 1) * 4, outer, 0)

    def convert(k, _):
        for j in range(16):
            xs[pl.ds(pl.multiple_of(k * 64, 64), 64), j * 128 : (j + 1) * 128] = (
                tall[pl.ds(k * 8, 8), j * 8 : (j + 1) * 8, :].reshape(64, 128).astype(BF16)
            )
        return 0

    lax.fori_loop(0, 16, convert, 0)

    for j in range(0, 16, 2):
        part = dot(w_ref[...], xs[:, j * 128 : (j + 2) * 128], TN)
        part = (part * (1.0 / 256) + bias).astype(BF16)
        for jj in range(2):
            for d in range(4):
                pair_ref[d, j + jj] = part[d * 32 : (d + 1) * 32, jj * 128 : (jj + 1) * 128]

    def weight(k, _):
        at = pl.multiple_of(k * 256, 256)
        gw_ref[pl.ds(at, 256), :] = dot(xs[pl.ds(at, 256), :], st_ref[...], NT).astype(BF16)
        return 0

    lax.fori_loop(0, 4, weight, 0)


def outer_call(lt, rt, st, w, bias):
    return pl.pallas_call(
        outer_kernel,
        out_shape=(
            jax.ShapeDtypeStruct((4, 16, 32, 128), BF16),
            jax.ShapeDtypeStruct((1024, 128), BF16),
        ),
        in_specs=(*hbm(1), *vmem(4)),
        out_specs=tuple(vmem(2)),
        scratch_shapes=[
            pltpu.VMEM((128, 128, 128), F32),
            pltpu.VMEM((1024, 2048), BF16),
            pltpu.VMEM((4096, 256), BF16),
            pltpu.SemaphoreType.DMA((4,)),
        ],
        cost_estimate=cost(11),
        name="outer",
    )(lt, rt, st, w, bias)


def back_kernel(
    gl_ref, gr_ref, normed_ref, wt_ref, count_ref, gw_ref,
    grad_ref, all_ref,
    sums, flat_ref,
):
    own = 16
    left = gl_ref[0].astype(F32)
    for k in range(1, 16):
        left = left + gl_ref[k].astype(F32)
    right = gr_ref[...].astype(F32)
    sums[0:256, :] = left.reshape(256, 128)
    sums[256:512, :] = right.reshape(256, 128)
    for i in range(own):
        t = [sums[pl.ds(side * 256 + i, 16, stride=own), :] for side in range(2)]
        grad_ref[:, i * 64 : (i + 1) * 64] = jnp.concatenate(
            [t[0][:, :64], t[0][:, 64:], t[1][:, :64], t[1][:, 64:]], axis=0
        ).astype(BF16)
    grad = grad_ref[...]
    both = dot(grad, normed_ref[...], NN)
    wt = wt_ref[...].astype(F32)
    column = jnp.sum(grad.astype(F32), axis=1, keepdims=True)
    gain = jnp.sum(both[:, 256:] * wt, axis=0, keepdims=True)
    shift = jnp.sum(column * wt, axis=0, keepdims=True)
    on = lax.broadcasted_iota(jnp.int32, (64, 128), 0) == lax.broadcasted_iota(
        jnp.int32, (64, 128), 1
    )
    bias = jnp.sum(jnp.where(on, column, 0.0), axis=0, keepdims=True)
    rows = [
        count_ref[...], gain[:, :128], gain[:, 128:], shift[:, :128], shift[:, 128:], bias,
    ]
    flat_ref[...] = jnp.zeros((16, 16, 128), F32)
    for k in range(8):
        flat_ref[k, 0:8, :] = both[k * 8 : (k + 1) * 8, :128]
        flat_ref[8 + k, 0:8, :] = both[k * 8 : (k + 1) * 8, 128:256]
    for k, row in enumerate(rows):
        hi = row.astype(BF16).astype(F32)
        flat_ref[k, 8:9, :] = hi
        flat_ref[k, 9:10, :] = row - hi
    for k in range(16):
        all_ref[k, 0:64, :] = gw_ref[k * 64 : (k + 1) * 64, :]
        all_ref[k, 64:80, :] = flat_ref[k].astype(BF16)


def back_call(gl, gr, normed, wt, count, gw):
    return pl.pallas_call(
        back_kernel,
        out_shape=(
            jax.ShapeDtypeStruct((64, 1024), BF16),
            jax.ShapeDtypeStruct((16, 80, 128), BF16),
        ),
        in_specs=vmem(6),
        out_specs=tuple(vmem(2)),
        scratch_shapes=[pltpu.VMEM((512, 128), F32), pltpu.VMEM((16, 16, 128), F32)],
        compiler_params=limit(8),
        cost_estimate=cost(2),
        name="back",
    )(gl, gr, normed, wt, count, gw)


def norm_kernel(x_ref, gain_ref, wt_ref, grad_ref, gx_ref, rows, rstds):
    seqs, own = 64, 16
    gain = gain_ref[...]

    def block(k, _):
        x = x_ref[pl.ds(k * 128, 128), :].astype(F32)
        mean = jnp.mean(x, axis=-1, keepdims=True)
        centre = x - mean
        spread = jnp.mean(centre * centre, axis=-1, keepdims=True)
        rstd = lax.rsqrt(spread + EPSILON)
        y = centre * rstd
        rows[0, pl.ds(k * 128, 128), :] = y[:, :128]
        rows[1, pl.ds(k * 128, 128), :] = y[:, 128:]
        rstds[pl.ds(k * 128, 128), :] = jnp.broadcast_to(rstd, (128, 128))
        return 0

    lax.fori_loop(0, 8, block, 0)
    for i in range(own):
        gn = dot(grad_ref[:, i * seqs : (i + 1) * seqs], wt_ref[...], TN)
        hat = jnp.concatenate(
            [rows[h, pl.ds(i, seqs, stride=own), :] for h in range(2)], axis=1
        )
        rstd = rstds[pl.ds(i, seqs, stride=own), :][:, :1]
        g = gn * gain
        a = jnp.mean(g, axis=-1, keepdims=True)
        b = jnp.mean(g * hat, axis=-1, keepdims=True)
        gx = rstd * (g - a - hat * b)
        for h in range(2):
            rows[h, pl.ds(i, seqs, stride=own), :] = gx[:, h * 128 : (h + 1) * 128]
    for h in range(2):
        gx_ref[:, h * 128 : (h + 1) * 128] = rows[h].astype(BF16)


def norm_call(x, gain, wt, grad):
    return pl.pallas_call(
        norm_kernel,
        out_shape=jax.ShapeDtypeStruct((1024, 256), BF16),
        in_specs=vmem(4),
        out_specs=pl.BlockSpec(memory_space=pltpu.VMEM),
        scratch_shapes=[pltpu.VMEM((2, 1024, 128), F32), pltpu.VMEM((1024, 128), F32)],
        compiler_params=limit(8),
        cost_estimate=cost(5),
        name="norm",
    )(x, gain, wt, grad)


def exchange(value, axis):
    return lax.all_to_all(value, axis, 0, 0, tiled=True)


def swap(value):
    return lax.ppermute(value, "col_1", [(0, 1), (1, 0)])


def place(d, r, c):
    return (d * 4 + r) * 8 + c


def right_pairs():
    return [
        (place(y, r, c), place(c % 4, y, 2 * r + c // 4))
        for y in range(4)
        for r in range(4)
        for c in range(8)
    ]


def rotate(value, axis, by):
    return lax.ppermute(value, axis, [(k, (k + by) % 4) for k in range(4)])


EVERY = ("depth", "row", "col_0", "col_1")
PLANE = ("depth", "row")


def summed(parts):
    return jnp.sum(parts.astype(F32), axis=0)


def give_kernel(a_ref, b_ref, out_ref):
    total = a_ref[...] + b_ref[...]
    row = total[72:73] + total[73:74]
    hi = row.astype(BF16).astype(F32)
    at = lax.broadcasted_iota(jnp.int32, (8, 128), 0)
    tail = jnp.where(at == 0, hi, jnp.where(at == 1, row - hi, 0.0))
    chunk = jnp.concatenate([total[:72], tail], axis=0).astype(BF16)
    for k in range(16):
        out_ref[k] = chunk


def give_call(a, b):
    return pl.pallas_call(
        give_kernel,
        out_shape=jax.ShapeDtypeStruct((16, 80, 128), BF16),
        in_specs=vmem(2),
        out_specs=vmem(1)[0],
        compiler_params=limit(2),
        cost_estimate=cost(1),
        name="give",
    )(a, b)


def finish_kernel(all_ref, gw_ref, pw_ref, pb_ref, ob_ref, gain_ref, shift_ref):
    for k in range(16):
        gw_ref[k * 64 : (k + 1) * 64, :] = all_ref[k, 0:64, :].astype(F32)
    rows = []
    for k in range(8):
        for half in range(2):
            pw_ref[k * 8 : (k + 1) * 8, half * 128 : (half + 1) * 128] = all_ref[
                half * 8 + k, 64:72, :
            ].astype(F32)
        tail = all_ref[k, 72:80, :].astype(F32)
        rows.append(tail[0:1] + tail[1:2])
    ob_ref[...] = rows[0]
    gain_ref[...] = jnp.concatenate(rows[1:3], axis=1)
    shift_ref[...] = jnp.concatenate(rows[3:5], axis=1)
    pb_ref[...] = rows[5][:, :64]


def finish_call(total):
    return pl.pallas_call(
        finish_kernel,
        out_shape=(
            jax.ShapeDtypeStruct((1024, 128), F32),
            jax.ShapeDtypeStruct((64, 256), F32),
            jax.ShapeDtypeStruct((1, 64), F32),
            jax.ShapeDtypeStruct((1, 128), F32),
            jax.ShapeDtypeStruct((1, 256), F32),
            jax.ShapeDtypeStruct((1, 256), F32),
        ),
        in_specs=vmem(1),
        out_specs=tuple(vmem(6)),
        compiler_params=limit(4),
        cost_estimate=cost(1),
        name="finish",
    )(total)


def step(
    alignment, norm_gain, norm_shift, proj_weight, proj_bias, out_weight, out_bias, cotangent
):
    x = alignment.reshape(1024, 256)
    gain = norm_gain.reshape(1, 256)
    shift = norm_shift.reshape(1, 256)
    wt = proj_weight.T
    cot = exchange(jnp.transpose(cotangent, (1, 2, 0)).reshape(4, 16, 32, 128), "depth")
    left, right, normed = sides_call(x, gain, shift, wt, proj_bias.reshape(1, 64))
    pairs = right_pairs()
    near = exchange(left, ("depth", "col_0"))
    rights = [lax.ppermute(right, EVERY, pairs)]
    for m in range(1, 4):
        rights.append(rotate(rights[0], "row", m))
    far = swap(near)

    gp, st, count = grad_call(cot, out_weight)
    keep, send, rt = left_call(rights, gp)
    came = swap(send)
    mine = (keep.astype(F32) + came.astype(F32)).astype(BF16)
    lefts = exchange(mine, ("depth", "col_0"))

    *gr, lt = right_call(near, far, gp)
    for m in range(1, 4):
        gr[m] = rotate(gr[m], "row", m)
    right_grad = sum(g.astype(F32) for g in gr).astype(BF16)
    right_grad = lax.ppermute(right_grad, EVERY, [(b, a) for a, b in pairs])

    pair, gw = outer_call(lt, rt, st, out_weight, out_bias.reshape(1, 128))
    grad, total = back_call(lefts, right_grad, normed, wt, count, gw)

    total = exchange(total, PLANE)
    total = summed(total)
    for m in (1, 3):
        total = total + lax.ppermute(total, "col_0", [(k, k ^ m) for k in range(4)])
    other = swap(total)
    total = give_call(total, other)
    total = exchange(total, PLANE)
    gx = norm_call(x, gain, wt, grad)
    pair = exchange(pair, "depth")
    gw, gpw, gpb, gb, gg, gs = finish_call(total)
    return (
        jnp.transpose(pair.reshape(64, 32, 128), (2, 0, 1)),
        gx.reshape(alignment.shape),
        gpw.T,
        gpb.reshape(64),
        gw,
        gb.reshape(128),
        gg.reshape(256),
        gs.reshape(256),
    )


def solution(mesh):
    split = Mesh(mesh.devices.reshape(4, 4, 4, 2), EVERY)
    side = P("depth", ("row", "col_0", "col_1"), None)
    block = P("row", ("col_0", "col_1"), "depth")
    return jax.shard_map(
        step,
        mesh=split,
        in_specs=(side, P(), P(), P(), P(), P(), P(), block),
        out_specs=(block, side, P(), P(), P(), P(), P(), P()),
        check_vma=False,
    )
```

```python
import jax
import jax.numpy as jnp
from jax import lax
from jax.experimental import pallas as pl
from jax.experimental.pallas import tpu as pltpu
from jax.sharding import Mesh
from jax.sharding import PartitionSpec as P

EPSILON = 1e-05
F32 = jnp.float32
BF16 = jnp.bfloat16
NN = (((1,), (0,)), ((), ()))
NT = (((1,), (1,)), ((), ()))
TN = (((0,), (0,)), ((), ()))


def dot(a, b, dims):
    return lax.dot_general(a, b, dims, preferred_element_type=F32)


def vmem(count):
    return [pl.BlockSpec(memory_space=pltpu.VMEM)] * count


def hbm(count):
    return [pl.BlockSpec(memory_space=pltpu.HBM)] * count


def cost(us):
    return pl.CostEstimate(flops=us * 400_000_000, bytes_accessed=1_000_000, transcendentals=0)


def limit(mib):
    return pltpu.CompilerParams(vmem_limit_bytes=mib * 2**20)


def column_of(row):
    size = row.shape[1]
    on = lax.broadcasted_iota(jnp.int32, (size, size), 0) == lax.broadcasted_iota(
        jnp.int32, (size, size), 1
    )
    return jnp.sum(jnp.where(on, row, 0.0), axis=1, keepdims=True)


def sides_kernel(
    x_ref, gain_ref, shift_ref, wt_ref, bias_ref, left_ref, right_ref, normed_ref, rows, packed
):
    seqs, own = 64, 16
    gain, shift = gain_ref[...], shift_ref[...]

    def block(k, _):
        x = x_ref[pl.ds(k * 128, 128), :].astype(F32)
        centre = x - jnp.mean(x, axis=-1, keepdims=True)
        spread = jnp.mean(centre * centre, axis=-1, keepdims=True)
        hat = centre * lax.rsqrt(spread + EPSILON)
        rows[0, pl.ds(k * 128, 128), :] = hat[:, :128]
        rows[1, pl.ds(k * 128, 128), :] = hat[:, 128:]
        return 0

    lax.fori_loop(0, 8, block, 0)
    for i in range(own):
        hat = jnp.concatenate(
            [rows[h, pl.ds(i, seqs, stride=own), :] for h in range(2)], axis=1
        )
        at = slice(i * seqs, (i + 1) * seqs)
        normed_ref[at, :256] = (hat * gain + shift).astype(BF16)
        normed_ref[at, 256:] = hat.astype(BF16)
    sides = dot(wt_ref[...], normed_ref[:, :256], NT) + column_of(bias_ref[...])
    for i in range(own):
        t = sides[:, i * seqs : (i + 1) * seqs]
        for side in range(2):
            lo = t[side * 32 : side * 32 + 16]
            hi = t[side * 32 + 16 : side * 32 + 32]
            packed[pl.ds(side * 256 + i, 16, stride=own), :] = jnp.concatenate([lo, hi], axis=1)
    left = packed[:256, :].astype(BF16).reshape(16, own, 128)
    for peer in range(16):
        left_ref[peer] = left
    right_ref[...] = packed[256:, :].astype(BF16).reshape(16, own, 128)


def sides_call(x, gain, shift, wt, bias):
    return pl.pallas_call(
        sides_kernel,
        out_shape=(
            jax.ShapeDtypeStruct((16, 16, 16, 128), BF16),
            jax.ShapeDtypeStruct((16, 16, 128), BF16),
            jax.ShapeDtypeStruct((1024, 512), BF16),
        ),
        in_specs=vmem(5),
        out_specs=tuple(vmem(3)),
        scratch_shapes=[pltpu.VMEM((2, 1024, 128), F32), pltpu.VMEM((512, 128), F32)],
        cost_estimate=cost(4),
        name="sides",
    )(x, gain, shift, wt, bias)


def grad_kernel(s_ref, w_ref, gp_ref, st_ref, gb_ref, tall, held, sems):
    ones = lax.broadcasted_iota(jnp.int32, (128, 128), 0) == lax.broadcasted_iota(
        jnp.int32, (128, 128), 1
    )
    columns = []
    for d in range(4):
        count = jnp.zeros((32, 128), F32)
        for j in range(16):
            t = s_ref[d, j].astype(F32)
            count = count + t
            st_ref[d * 32 : (d + 1) * 32, j * 128 : (j + 1) * 128] = (t * (1.0 / 256)).astype(
                BF16
            )
        columns.append(jnp.sum(count, axis=1, keepdims=True))
    column = jnp.concatenate(columns, axis=0)
    gb_ref[...] = jnp.sum(jnp.where(ones, column, 0.0), axis=0, keepdims=True)

    for j in range(0, 16, 2):
        g = dot(w_ref[...], st_ref[:, j * 128 : (j + 2) * 128], NN)
        for jj in range(2):
            tall[:, (j + jj) * 8 : (j + jj + 1) * 8, :] = g[
                :, jj * 128 : (jj + 1) * 128
            ].reshape(128, 8, 128)

    def relay(c, _):
        for e in range(32):
            held[c, e * 16 : (e + 1) * 16, :] = tall[
                c * 4 + e // 8, pl.ds(e % 8, 16, stride=8), :
            ].astype(BF16)
        return 0

    copies = []
    for q in range(4):
        lax.fori_loop(q * 8, (q + 1) * 8, relay, 0)
        part = pl.ds(q * 8, 8)
        copies.append(pltpu.make_async_copy(held.at[part], gp_ref.at[part], sems.at[q]))
        copies[-1].start()
    for copy in copies:
        copy.wait()


def grad_call(s, w):
    return pl.pallas_call(
        grad_kernel,
        out_shape=(
            jax.ShapeDtypeStruct((32, 512, 128), BF16),
            jax.ShapeDtypeStruct((128, 2048), BF16),
            jax.ShapeDtypeStruct((1, 128), F32),
        ),
        in_specs=vmem(2),
        out_specs=(*hbm(1), *vmem(2)),
        scratch_shapes=[
            pltpu.VMEM((128, 128, 128), F32),
            pltpu.VMEM((32, 512, 128), BF16),
            pltpu.SemaphoreType.DMA((4,)),
        ],
        cost_estimate=cost(5),
        name="grad",
    )(s, w)


def left_kernel(
    r0_ref, r1_ref, r2_ref, r3_ref, gp_ref, keep_ref, send_ref, rt_ref,
    rbuf, held, sems, keep, send, out_sems,
):
    copies = []
    for q in range(8):
        part = pl.ds((q // 2 + q % 2 * 4) * 4, 4)
        copies.append(pltpu.make_async_copy(gp_ref.at[part], held.at[part], sems.at[q]))
        copies[-1].start()
    core = lax.axis_index("col_1")
    row = lax.axis_index("row")
    for m, ref in enumerate((r0_ref, r1_ref, r2_ref, r3_ref)):
        rbuf[lax.rem(row - m + 4, 4)] = ref[...].reshape(256, 128)
    for eh in range(2):
        for half in range(2):
            cut = [rbuf[2 * half + y][:, eh * 64 : eh * 64 + 64] for y in range(2)]
            rt_ref[eh * 256 : (eh + 1) * 256, half * 128 : (half + 1) * 128] = jnp.concatenate(
                cut, axis=1
            )

    def left(k, _):
        sums = [dot(held[ch * 16 + k], rt_ref[...], TN) for ch in range(2)]
        for y in range(4):
            t = jnp.concatenate([v[:, y * 64 : (y + 1) * 64] for v in sums], axis=1)
            for z in range(4):
                a = t[z * 32 : z * 32 + 16]
                b = t[z * 32 + 16 : z * 32 + 32]
                keep[y * 4 + z, k] = jnp.where(core == 0, a, b).astype(BF16)
                send[y * 4 + z, k] = jnp.where(core == 0, b, a).astype(BF16)
        return 0

    outs = []
    for q in range(4):
        copies[2 * q].wait()
        copies[2 * q + 1].wait()
        lax.fori_loop(q * 4, (q + 1) * 4, left, 0)
        part = pl.ds(q * 4, 4)
        outs.append(pltpu.make_async_copy(send.at[:, part], send_ref.at[:, part], out_sems.at[2 * q]))
        outs.append(pltpu.make_async_copy(keep.at[:, part], keep_ref.at[:, part], out_sems.at[2 * q + 1]))
        outs[-2].start()
        outs[-1].start()
    for copy in outs:
        copy.wait()


def left_call(rs, gp):
    return pl.pallas_call(
        left_kernel,
        out_shape=(
            jax.ShapeDtypeStruct((16, 16, 16, 128), BF16),
            jax.ShapeDtypeStruct((16, 16, 16, 128), BF16),
            jax.ShapeDtypeStruct((512, 256), BF16),
        ),
        in_specs=(*vmem(4), *hbm(1)),
        out_specs=(*hbm(2), *vmem(1)),
        scratch_shapes=[
            pltpu.VMEM((4, 256, 128), BF16),
            pltpu.VMEM((32, 512, 128), BF16),
            pltpu.SemaphoreType.DMA((8,)),
            pltpu.VMEM((16, 16, 16, 128), BF16),
            pltpu.VMEM((16, 16, 16, 128), BF16),
            pltpu.SemaphoreType.DMA((8,)),
        ],
        cost_estimate=cost(5),
        name="left",
    )(*rs, gp)


def right_kernel(
    near_ref, far_ref, gp_ref, g0_ref, g1_ref, g2_ref, g3_ref, lt_ref,
    gbuf, held, sems, near, far, lt,
):
    sides = [
        pltpu.make_async_copy(near_ref, near, sems.at[4]),
        pltpu.make_async_copy(far_ref, far, sems.at[5]),
    ]
    for copy in sides:
        copy.start()
    copies = []
    for q in range(4):
        part = pl.ds(q * 8, 8)
        copies.append(pltpu.make_async_copy(gp_ref.at[part], held.at[part], sems.at[q]))
        copies[-1].start()
    for copy in sides:
        copy.wait()
    core = lax.axis_index("col_1")
    row = lax.axis_index("row")

    def merge(k, _):
        for ref, side in ((near, core), (far, 1 - core)):
            for z in range(4):
                parts = [ref[y * 4 + z, k] for y in range(4)]
                for ch in range(2):
                    cut = [p[:, ch * 64 : ch * 64 + 64] for p in parts]
                    at = pl.multiple_of((ch * 16 + k) * 128 + (2 * z + side) * 16, 16)
                    lt[pl.ds(at, 16), 0:128] = jnp.concatenate(cut[:2], axis=1)
                    lt[pl.ds(at, 16), 128:256] = jnp.concatenate(cut[2:], axis=1)
        return 0

    lax.fori_loop(0, 16, merge, 0)
    kept = pltpu.make_async_copy(lt, lt_ref, sems.at[6])
    kept.start()

    for copy in copies:
        copy.wait()
    wide = jnp.concatenate([held[c] for c in range(32)], axis=1)
    total = dot(wide, lt[...], NN)
    for y in range(4):
        t = jnp.concatenate(
            [total[eh * 256 : (eh + 1) * 256, y * 64 : (y + 1) * 64] for eh in range(2)], axis=1
        )
        gbuf[y] = t.astype(BF16)
    for m, ref in enumerate((g0_ref, g1_ref, g2_ref, g3_ref)):
        ref[...] = gbuf[lax.rem(row + m, 4)].reshape(16, 16, 128)
    kept.wait()


def right_call(near, far, gp):
    return pl.pallas_call(
        right_kernel,
        out_shape=(
            *[jax.ShapeDtypeStruct((16, 16, 128), BF16)] * 4,
            jax.ShapeDtypeStruct((4096, 256), BF16),
        ),
        in_specs=hbm(3),
        out_specs=(*vmem(4), *hbm(1)),
        scratch_shapes=[
            pltpu.VMEM((4, 256, 128), BF16),
            pltpu.VMEM((32, 512, 128), BF16),
            pltpu.SemaphoreType.DMA((7,)),
            pltpu.VMEM((16, 16, 16, 128), BF16),
            pltpu.VMEM((16, 16, 16, 128), BF16),
            pltpu.VMEM((4096, 256), BF16),
        ],
        cost_estimate=cost(5),
        name="right",
    )(near, far, gp)


def outer_kernel(
    lt_ref, rt_ref, st_ref, w_ref, bias_ref,
    p0_ref, p1_ref, p2_ref, p3_ref, gw_ref,
    tall, xs, lt, sems, pair,
):
    depth = lax.axis_index("depth")
    copies = []
    for q in range(4):
        part = pl.ds(q * 1024, 1024)
        copies.append(pltpu.make_async_copy(lt_ref.at[part], lt.at[part], sems.at[q]))
        copies[-1].start()
    bias = column_of(bias_ref[...])

    def outer(k, _):
        both = lt[pl.ds(pl.multiple_of(k * 256, 256), 256), :]
        o = dot(rt_ref[...], both, NT)
        for ch in range(2):
            for e in range(32):
                tall[k * 8 + ch * 4 + e // 8, pl.ds(e % 8, 16, stride=8), :] = o[
                    e * 16 : (e + 1) * 16, ch * 128 : (ch + 1) * 128
                ]
        return 0

    for q in range(4):
        copies[q].wait()
        lax.fori_loop(q * 4, (q + 1) * 4, outer, 0)

    def convert(k, _):
        for j in range(16):
            xs[pl.ds(pl.multiple_of(k * 64, 64), 64), j * 128 : (j + 1) * 128] = (
                tall[pl.ds(k * 8, 8), j * 8 : (j + 1) * 8, :].reshape(64, 128).astype(BF16)
            )
        return 0

    lax.fori_loop(0, 16, convert, 0)

    for j in range(0, 16, 2):
        part = dot(w_ref[...], xs[:, j * 128 : (j + 2) * 128], TN)
        part = (part * (1.0 / 256) + bias).astype(BF16)
        for jj in range(2):
            for d in range(4):
                pair[lax.rem(d - depth + 4, 4), j + jj] = part[
                    d * 32 : (d + 1) * 32, jj * 128 : (jj + 1) * 128
                ]
    for m, ref in enumerate((p0_ref, p1_ref, p2_ref, p3_ref)):
        ref[...] = pair[m]

    def weight(k, _):
        at = pl.multiple_of(k * 256, 256)
        gw_ref[pl.ds(at, 256), :] = dot(xs[pl.ds(at, 256), :], st_ref[...], NT).astype(BF16)
        return 0

    lax.fori_loop(0, 4, weight, 0)


def outer_call(lt, rt, st, w, bias):
    return pl.pallas_call(
        outer_kernel,
        out_shape=(
            *[jax.ShapeDtypeStruct((16, 32, 128), BF16)] * 4,
            jax.ShapeDtypeStruct((1024, 128), BF16),
        ),
        in_specs=(*hbm(1), *vmem(4)),
        out_specs=tuple(vmem(5)),
        scratch_shapes=[
            pltpu.VMEM((128, 128, 128), F32),
            pltpu.VMEM((1024, 2048), BF16),
            pltpu.VMEM((4096, 256), BF16),
            pltpu.SemaphoreType.DMA((4,)),
            pltpu.VMEM((4, 16, 32, 128), BF16),
        ],
        cost_estimate=cost(11),
        name="outer",
    )(lt, rt, st, w, bias)


def back_kernel(
    gl_ref, gr_ref, normed_ref, wt_ref, count_ref, gw_ref,
    grad_ref, all_ref,
    sums, flat_ref,
):
    own = 16
    left = gl_ref[0].astype(F32)
    for k in range(1, 16):
        left = left + gl_ref[k].astype(F32)
    right = gr_ref[...].astype(F32)
    sums[0:256, :] = left.reshape(256, 128)
    sums[256:512, :] = right.reshape(256, 128)
    for i in range(own):
        t = [sums[pl.ds(side * 256 + i, 16, stride=own), :] for side in range(2)]
        grad_ref[:, i * 64 : (i + 1) * 64] = jnp.concatenate(
            [t[0][:, :64], t[0][:, 64:], t[1][:, :64], t[1][:, 64:]], axis=0
        ).astype(BF16)
    grad = grad_ref[...]
    both = dot(grad, normed_ref[...], NN)
    wt = wt_ref[...].astype(F32)
    column = jnp.sum(grad.astype(F32), axis=1, keepdims=True)
    gain = jnp.sum(both[:, 256:] * wt, axis=0, keepdims=True)
    shift = jnp.sum(column * wt, axis=0, keepdims=True)
    on = lax.broadcasted_iota(jnp.int32, (64, 128), 0) == lax.broadcasted_iota(
        jnp.int32, (64, 128), 1
    )
    bias = jnp.sum(jnp.where(on, column, 0.0), axis=0, keepdims=True)
    rows = [
        count_ref[...], gain[:, :128], gain[:, 128:], shift[:, :128], shift[:, 128:], bias,
    ]
    flat_ref[...] = jnp.zeros((16, 16, 128), F32)
    for k in range(8):
        flat_ref[k, 0:8, :] = both[k * 8 : (k + 1) * 8, :128]
        flat_ref[8 + k, 0:8, :] = both[k * 8 : (k + 1) * 8, 128:256]
    for k, row in enumerate(rows):
        hi = row.astype(BF16).astype(F32)
        flat_ref[k, 8:9, :] = hi
        flat_ref[k, 9:10, :] = row - hi
    for k in range(16):
        all_ref[k, 0:64, :] = gw_ref[k * 64 : (k + 1) * 64, :]
        all_ref[k, 64:80, :] = flat_ref[k].astype(BF16)


def back_call(gl, gr, normed, wt, count, gw):
    return pl.pallas_call(
        back_kernel,
        out_shape=(
            jax.ShapeDtypeStruct((64, 1024), BF16),
            jax.ShapeDtypeStruct((16, 80, 128), BF16),
        ),
        in_specs=vmem(6),
        out_specs=tuple(vmem(2)),
        scratch_shapes=[pltpu.VMEM((512, 128), F32), pltpu.VMEM((16, 16, 128), F32)],
        compiler_params=limit(8),
        cost_estimate=cost(2),
        name="back",
    )(gl, gr, normed, wt, count, gw)


def norm_kernel(
    x_ref, gain_ref, wt_ref, grad_ref, p0_ref, p1_ref, p2_ref, p3_ref,
    gx_ref, pair_ref,
    rows, rstds,
):
    seqs, own = 64, 16
    depth = lax.axis_index("depth")
    for m, ref in enumerate((p0_ref, p1_ref, p2_ref, p3_ref)):
        pair_ref[pl.ds(lax.rem(depth - m + 4, 4) * 16, 16)] = ref[...]
    gain = gain_ref[...]

    def block(k, _):
        x = x_ref[pl.ds(k * 128, 128), :].astype(F32)
        mean = jnp.mean(x, axis=-1, keepdims=True)
        centre = x - mean
        spread = jnp.mean(centre * centre, axis=-1, keepdims=True)
        rstd = lax.rsqrt(spread + EPSILON)
        y = centre * rstd
        rows[0, pl.ds(k * 128, 128), :] = y[:, :128]
        rows[1, pl.ds(k * 128, 128), :] = y[:, 128:]
        rstds[pl.ds(k * 128, 128), :] = jnp.broadcast_to(rstd, (128, 128))
        return 0

    lax.fori_loop(0, 8, block, 0)
    for i in range(own):
        gn = dot(grad_ref[:, i * seqs : (i + 1) * seqs], wt_ref[...], TN)
        hat = jnp.concatenate(
            [rows[h, pl.ds(i, seqs, stride=own), :] for h in range(2)], axis=1
        )
        rstd = rstds[pl.ds(i, seqs, stride=own), :][:, :1]
        g = gn * gain
        a = jnp.mean(g, axis=-1, keepdims=True)
        b = jnp.mean(g * hat, axis=-1, keepdims=True)
        gx = rstd * (g - a - hat * b)
        for h in range(2):
            rows[h, pl.ds(i, seqs, stride=own), :] = gx[:, h * 128 : (h + 1) * 128]
    for h in range(2):
        gx_ref[:, h * 128 : (h + 1) * 128] = rows[h].astype(BF16)


def norm_call(x, gain, wt, grad, pair):
    return pl.pallas_call(
        norm_kernel,
        out_shape=(
            jax.ShapeDtypeStruct((1024, 256), BF16),
            jax.ShapeDtypeStruct((64, 32, 128), BF16),
        ),
        in_specs=vmem(8),
        out_specs=tuple(vmem(2)),
        scratch_shapes=[pltpu.VMEM((2, 1024, 128), F32), pltpu.VMEM((1024, 128), F32)],
        compiler_params=limit(10),
        cost_estimate=cost(5),
        name="norm",
    )(x, gain, wt, grad, *pair)


def exchange(value, axis):
    return lax.all_to_all(value, axis, 0, 0, tiled=True)


def swap(value):
    return lax.ppermute(value, "col_1", [(0, 1), (1, 0)])


def place(d, r, c):
    return (d * 4 + r) * 8 + c


def right_pairs():
    return [
        (place(y, r, c), place(c % 4, y, 2 * r + c // 4))
        for y in range(4)
        for r in range(4)
        for c in range(8)
    ]


def rotate(value, axis, by):
    return lax.ppermute(value, axis, [(k, (k + by) % 4) for k in range(4)])


EVERY = ("depth", "row", "col_0", "col_1")
PLANE = ("depth", "row")


def summed(parts):
    return jnp.sum(parts.astype(F32), axis=0)


def give_kernel(a_ref, b_ref, out_ref):
    total = a_ref[...] + b_ref[...]
    row = total[72:73] + total[73:74]
    hi = row.astype(BF16).astype(F32)
    at = lax.broadcasted_iota(jnp.int32, (8, 128), 0)
    tail = jnp.where(at == 0, hi, jnp.where(at == 1, row - hi, 0.0))
    chunk = jnp.concatenate([total[:72], tail], axis=0).astype(BF16)
    for k in range(16):
        out_ref[k] = chunk


def give_call(a, b):
    return pl.pallas_call(
        give_kernel,
        out_shape=jax.ShapeDtypeStruct((16, 80, 128), BF16),
        in_specs=vmem(2),
        out_specs=vmem(1)[0],
        compiler_params=limit(2),
        cost_estimate=cost(1),
        name="give",
    )(a, b)


def finish_kernel(all_ref, gw_ref, pw_ref, pb_ref, ob_ref, gain_ref, shift_ref):
    for k in range(16):
        gw_ref[k * 64 : (k + 1) * 64, :] = all_ref[k, 0:64, :].astype(F32)
    rows = []
    for k in range(8):
        for half in range(2):
            pw_ref[k * 8 : (k + 1) * 8, half * 128 : (half + 1) * 128] = all_ref[
                half * 8 + k, 64:72, :
            ].astype(F32)
        tail = all_ref[k, 72:80, :].astype(F32)
        rows.append(tail[0:1] + tail[1:2])
    ob_ref[...] = rows[0]
    gain_ref[...] = jnp.concatenate(rows[1:3], axis=1)
    shift_ref[...] = jnp.concatenate(rows[3:5], axis=1)
    pb_ref[...] = rows[5][:, :64]


def finish_call(total):
    return pl.pallas_call(
        finish_kernel,
        out_shape=(
            jax.ShapeDtypeStruct((1024, 128), F32),
            jax.ShapeDtypeStruct((64, 256), F32),
            jax.ShapeDtypeStruct((1, 64), F32),
            jax.ShapeDtypeStruct((1, 128), F32),
            jax.ShapeDtypeStruct((1, 256), F32),
            jax.ShapeDtypeStruct((1, 256), F32),
        ),
        in_specs=vmem(1),
        out_specs=tuple(vmem(6)),
        compiler_params=limit(4),
        cost_estimate=cost(1),
        name="finish",
    )(total)


def step(
    alignment, norm_gain, norm_shift, proj_weight, proj_bias, out_weight, out_bias, cotangent
):
    x = alignment.reshape(1024, 256)
    gain = norm_gain.reshape(1, 256)
    shift = norm_shift.reshape(1, 256)
    wt = proj_weight.T
    cot = exchange(jnp.transpose(cotangent, (1, 2, 0)).reshape(4, 16, 32, 128), "depth")
    left, right, normed = sides_call(x, gain, shift, wt, proj_bias.reshape(1, 64))
    pairs = right_pairs()
    near = exchange(left, ("depth", "col_0"))
    rights = [lax.ppermute(right, EVERY, pairs)]
    for m in range(1, 4):
        rights.append(rotate(rights[0], "row", m))
    far = swap(near)

    gp, st, count = grad_call(cot, out_weight)
    keep, send, rt = left_call(rights, gp)
    came = swap(send)
    mine = (keep.astype(F32) + came.astype(F32)).astype(BF16)
    lefts = exchange(mine, ("depth", "col_0"))

    *gr, lt = right_call(near, far, gp)
    for m in range(1, 4):
        gr[m] = rotate(gr[m], "row", m)
    right_grad = sum(g.astype(F32) for g in gr).astype(BF16)
    right_grad = lax.ppermute(right_grad, EVERY, [(b, a) for a, b in pairs])

    *pair, gw = outer_call(lt, rt, st, out_weight, out_bias.reshape(1, 128))
    grad, total = back_call(lefts, right_grad, normed, wt, count, gw)

    total = exchange(total, PLANE)
    total = summed(total)
    for m in (1, 3):
        total = total + lax.ppermute(total, "col_0", [(k, k ^ m) for k in range(4)])
    other = swap(total)
    total = give_call(total, other)
    total = exchange(total, PLANE)
    for m in range(1, 4):
        pair[m] = rotate(pair[m], "depth", m)
    gx, pair = norm_call(x, gain, wt, grad, pair)
    gw, gpw, gpb, gb, gg, gs = finish_call(total)
    return (
        jnp.transpose(pair, (2, 0, 1)),
        gx.reshape(alignment.shape),
        gpw.T,
        gpb.reshape(64),
        gw,
        gb.reshape(128),
        gg.reshape(256),
        gs.reshape(256),
    )


def solution(mesh):
    split = Mesh(mesh.devices.reshape(4, 4, 4, 2), EVERY)
    side = P("depth", ("row", "col_0", "col_1"), None)
    block = P("row", ("col_0", "col_1"), "depth")
    return jax.shard_map(
        step,
        mesh=split,
        in_specs=(side, P(), P(), P(), P(), P(), P(), block),
        out_specs=(block, side, P(), P(), P(), P(), P(), P()),
        check_vma=False,
    )
```

```python
import jax
import jax.numpy as jnp
from jax import lax
from jax.experimental import pallas as pl
from jax.experimental.pallas import tpu as pltpu
from jax.sharding import Mesh
from jax.sharding import PartitionSpec as P

EPSILON = 1e-05
F32 = jnp.float32
BF16 = jnp.bfloat16
NN = (((1,), (0,)), ((), ()))
NT = (((1,), (1,)), ((), ()))
TN = (((0,), (0,)), ((), ()))


def dot(a, b, dims):
    return lax.dot_general(a, b, dims, preferred_element_type=F32)


def vmem(count):
    return [pl.BlockSpec(memory_space=pltpu.VMEM)] * count


def hbm(count):
    return [pl.BlockSpec(memory_space=pltpu.HBM)] * count


def cost(us):
    return pl.CostEstimate(flops=us * 400_000_000, bytes_accessed=1_000_000, transcendentals=0)


def limit(mib):
    return pltpu.CompilerParams(vmem_limit_bytes=mib * 2**20)


def column_of(row):
    size = row.shape[1]
    on = lax.broadcasted_iota(jnp.int32, (size, size), 0) == lax.broadcasted_iota(
        jnp.int32, (size, size), 1
    )
    return jnp.sum(jnp.where(on, row, 0.0), axis=1, keepdims=True)


def sides_kernel(
    x_ref, gain_ref, shift_ref, wt_ref, bias_ref, left_ref, right_ref, normed_ref, rows, packed
):
    seqs, own = 64, 16
    gain, shift = gain_ref[...], shift_ref[...]

    def block(k, _):
        x = x_ref[pl.ds(k * 128, 128), :].astype(F32)
        centre = x - jnp.mean(x, axis=-1, keepdims=True)
        spread = jnp.mean(centre * centre, axis=-1, keepdims=True)
        hat = centre * lax.rsqrt(spread + EPSILON)
        rows[0, pl.ds(k * 128, 128), :] = hat[:, :128]
        rows[1, pl.ds(k * 128, 128), :] = hat[:, 128:]
        return 0

    lax.fori_loop(0, 8, block, 0)
    for i in range(own):
        hat = jnp.concatenate(
            [rows[h, pl.ds(i, seqs, stride=own), :] for h in range(2)], axis=1
        )
        at = slice(i * seqs, (i + 1) * seqs)
        normed_ref[at, :256] = (hat * gain + shift).astype(BF16)
        normed_ref[at, 256:] = hat.astype(BF16)
    sides = dot(wt_ref[...], normed_ref[:, :256], NT) + column_of(bias_ref[...])
    for i in range(own):
        t = sides[:, i * seqs : (i + 1) * seqs]
        for side in range(2):
            lo = t[side * 32 : side * 32 + 16]
            hi = t[side * 32 + 16 : side * 32 + 32]
            packed[pl.ds(side * 256 + i, 16, stride=own), :] = jnp.concatenate([lo, hi], axis=1)
    left = packed[:256, :].astype(BF16).reshape(16, own, 128)
    for peer in range(16):
        left_ref[peer] = left
    right_ref[...] = packed[256:, :].astype(BF16).reshape(16, own, 128)


def sides_call(x, gain, shift, wt, bias):
    return pl.pallas_call(
        sides_kernel,
        out_shape=(
            jax.ShapeDtypeStruct((16, 16, 16, 128), BF16),
            jax.ShapeDtypeStruct((16, 16, 128), BF16),
            jax.ShapeDtypeStruct((1024, 512), BF16),
        ),
        in_specs=vmem(5),
        out_specs=tuple(vmem(3)),
        scratch_shapes=[pltpu.VMEM((2, 1024, 128), F32), pltpu.VMEM((512, 128), F32)],
        cost_estimate=cost(4),
        name="sides",
    )(x, gain, shift, wt, bias)


def grad_kernel(s_ref, w_ref, gp_ref, st_ref, gb_ref, tall, held, st, sems):
    columns = []
    for d in range(4):
        count = jnp.zeros((32, 128), F32)
        for j in range(16):
            t = s_ref[d, j].astype(F32)
            count = count + t
            st[d * 32 : (d + 1) * 32, j * 128 : (j + 1) * 128] = (t * (1.0 / 256)).astype(BF16)
        columns.append(jnp.sum(count, axis=1, keepdims=True))
    copies = [pltpu.make_async_copy(st, st_ref, sems.at[8])]
    copies[0].start()

    def relay(c, _):
        for e in range(32):
            held[c, e * 16 : (e + 1) * 16, :] = tall[
                c * 4 + e // 8, pl.ds(e % 8 * 3, 16, stride=11), :
            ].astype(BF16)
        return 0

    for half in range(2):
        for j in range(0, 16, 2):
            g = dot(
                w_ref[half * 512 : (half + 1) * 512, :], st[:, j * 128 : (j + 2) * 128], NN
            )
            for jj in range(2):
                for q in range(64):
                    tall[half * 64 + q, pl.ds((j + jj) * 11, 8, stride=3), :] = g[
                        q * 8 : (q + 1) * 8, jj * 128 : (jj + 1) * 128
                    ]
        for q in range(half * 4, half * 4 + 4):
            lax.fori_loop(q * 4, (q + 1) * 4, relay, 0)
            part = pl.ds(q * 4, 4)
            copies.append(pltpu.make_async_copy(held.at[part], gp_ref.at[part], sems.at[q]))
            copies[-1].start()
    on = lax.broadcasted_iota(jnp.int32, (128, 128), 0) == lax.broadcasted_iota(
        jnp.int32, (128, 128), 1
    )
    column = jnp.concatenate(columns, axis=0)
    gb_ref[...] = jnp.sum(jnp.where(on, column, 0.0), axis=0, keepdims=True)
    for copy in copies:
        copy.wait()


def grad_call(s, w):
    return pl.pallas_call(
        grad_kernel,
        out_shape=(
            jax.ShapeDtypeStruct((32, 512, 128), BF16),
            jax.ShapeDtypeStruct((128, 2048), BF16),
            jax.ShapeDtypeStruct((1, 128), F32),
        ),
        in_specs=vmem(2),
        out_specs=(*hbm(2), *vmem(1)),
        scratch_shapes=[
            pltpu.VMEM((128, 192, 128), F32),
            pltpu.VMEM((32, 512, 128), BF16),
            pltpu.VMEM((128, 2048), BF16),
            pltpu.SemaphoreType.DMA((9,)),
        ],
        compiler_params=limit(59),
        cost_estimate=cost(5),
        name="grad",
    )(s, w)


def left_kernel(
    r0_ref, r1_ref, r2_ref, r3_ref, gp_ref, keep_ref, send_ref, rt_ref,
    rbuf, held, sems, keep, send, out_sems,
):
    copies = []
    for q in range(8):
        part = pl.ds((q // 2 + q % 2 * 4) * 4, 4)
        copies.append(pltpu.make_async_copy(gp_ref.at[part], held.at[part], sems.at[q]))
        copies[-1].start()
    core = lax.axis_index("col_1")
    row = lax.axis_index("row")
    for m, ref in enumerate((r0_ref, r1_ref, r2_ref, r3_ref)):
        rbuf[lax.rem(row - m + 4, 4)] = ref[...].reshape(256, 128)
    for eh in range(2):
        for half in range(2):
            cut = [rbuf[2 * half + y][:, eh * 64 : eh * 64 + 64] for y in range(2)]
            rt_ref[eh * 256 : (eh + 1) * 256, half * 128 : (half + 1) * 128] = jnp.concatenate(
                cut, axis=1
            )

    def left(k, _):
        sums = [dot(held[ch * 16 + k], rt_ref[...], TN) for ch in range(2)]
        for y in range(4):
            t = jnp.concatenate([v[:, y * 64 : (y + 1) * 64] for v in sums], axis=1)
            for z in range(4):
                a = t[z * 32 : z * 32 + 16]
                b = t[z * 32 + 16 : z * 32 + 32]
                keep[y * 4 + z, k] = jnp.where(core == 0, a, b).astype(BF16)
                send[y * 4 + z, k] = jnp.where(core == 0, b, a).astype(BF16)
        return 0

    outs = []
    for q in range(4):
        copies[2 * q].wait()
        copies[2 * q + 1].wait()
        lax.fori_loop(q * 4, (q + 1) * 4, left, 0)
        part = pl.ds(q * 4, 4)
        outs.append(pltpu.make_async_copy(send.at[:, part], send_ref.at[:, part], out_sems.at[2 * q]))
        outs.append(pltpu.make_async_copy(keep.at[:, part], keep_ref.at[:, part], out_sems.at[2 * q + 1]))
        outs[-2].start()
        outs[-1].start()
    for copy in outs:
        copy.wait()


def left_call(rs, gp):
    return pl.pallas_call(
        left_kernel,
        out_shape=(
            jax.ShapeDtypeStruct((16, 16, 16, 128), BF16),
            jax.ShapeDtypeStruct((16, 16, 16, 128), BF16),
            jax.ShapeDtypeStruct((512, 256), BF16),
        ),
        in_specs=(*vmem(4), *hbm(1)),
        out_specs=(*hbm(2), *vmem(1)),
        scratch_shapes=[
            pltpu.VMEM((4, 256, 128), BF16),
            pltpu.VMEM((32, 512, 128), BF16),
            pltpu.SemaphoreType.DMA((8,)),
            pltpu.VMEM((16, 16, 16, 128), BF16),
            pltpu.VMEM((16, 16, 16, 128), BF16),
            pltpu.SemaphoreType.DMA((8,)),
        ],
        compiler_params=limit(59),
        cost_estimate=cost(5),
        name="left",
    )(*rs, gp)


def right_kernel(
    near_ref, far_ref, gp_ref, g0_ref, g1_ref, g2_ref, g3_ref, lt_ref,
    gbuf, held, sems, near, far, lt,
):
    sides = [
        pltpu.make_async_copy(near_ref, near, sems.at[4]),
        pltpu.make_async_copy(far_ref, far, sems.at[5]),
    ]
    for copy in sides:
        copy.start()
    copies = []
    for q in range(4):
        part = pl.ds(q * 8, 8)
        copies.append(pltpu.make_async_copy(gp_ref.at[part], held.at[part], sems.at[q]))
        copies[-1].start()
    for copy in sides:
        copy.wait()
    core = lax.axis_index("col_1")
    row = lax.axis_index("row")

    def merge(k, _):
        for ref, side in ((near, core), (far, 1 - core)):
            for z in range(4):
                parts = [ref[y * 4 + z, k] for y in range(4)]
                for ch in range(2):
                    cut = [p[:, ch * 64 : ch * 64 + 64] for p in parts]
                    at = pl.multiple_of((ch * 16 + k) * 128 + (2 * z + side) * 16, 16)
                    lt[pl.ds(at, 16), 0:128] = jnp.concatenate(cut[:2], axis=1)
                    lt[pl.ds(at, 16), 128:256] = jnp.concatenate(cut[2:], axis=1)
        return 0

    lax.fori_loop(0, 16, merge, 0)
    kept = pltpu.make_async_copy(lt, lt_ref, sems.at[6])
    kept.start()

    for copy in copies:
        copy.wait()
    wide = jnp.concatenate([held[c] for c in range(32)], axis=1)
    total = dot(wide, lt[...], NN)
    for y in range(4):
        t = jnp.concatenate(
            [total[eh * 256 : (eh + 1) * 256, y * 64 : (y + 1) * 64] for eh in range(2)], axis=1
        )
        gbuf[y] = t.astype(BF16)
    for m, ref in enumerate((g0_ref, g1_ref, g2_ref, g3_ref)):
        ref[...] = gbuf[lax.rem(row + m, 4)].reshape(16, 16, 128)
    kept.wait()


def right_call(near, far, gp):
    return pl.pallas_call(
        right_kernel,
        out_shape=(
            *[jax.ShapeDtypeStruct((16, 16, 128), BF16)] * 4,
            jax.ShapeDtypeStruct((4096, 256), BF16),
        ),
        in_specs=hbm(3),
        out_specs=(*vmem(4), *hbm(1)),
        scratch_shapes=[
            pltpu.VMEM((4, 256, 128), BF16),
            pltpu.VMEM((32, 512, 128), BF16),
            pltpu.SemaphoreType.DMA((7,)),
            pltpu.VMEM((16, 16, 16, 128), BF16),
            pltpu.VMEM((16, 16, 16, 128), BF16),
            pltpu.VMEM((4096, 256), BF16),
        ],
        compiler_params=limit(59),
        cost_estimate=cost(5),
        name="right",
    )(near, far, gp)


def outer_kernel(
    lt_ref, rt_ref, st_ref, w_ref, bias_ref,
    p0_ref, p1_ref, p2_ref, p3_ref, gw_ref,
    tall, xs, lt, sems, pair, st, w, gw,
):
    depth = lax.axis_index("depth")
    late = [
        pltpu.make_async_copy(w_ref, w, sems.at[4]),
        pltpu.make_async_copy(st_ref, st, sems.at[5]),
    ]
    copies = []
    for q in range(4):
        part = pl.ds(q * 1024, 1024)
        copies.append(pltpu.make_async_copy(lt_ref.at[part], lt.at[part], sems.at[q]))
        copies[-1].start()
    for copy in late:
        copy.start()
    bias = column_of(bias_ref[...])

    def outer(k, _):
        both = lt[pl.ds(pl.multiple_of(k * 256, 256), 256), :]
        o = dot(rt_ref[...], both, NT)
        for ch in range(2):
            for e in range(32):
                tall[k * 8 + ch * 4 + e // 8, pl.ds(e % 8 * 3, 16, stride=11), :] = o[
                    e * 16 : (e + 1) * 16, ch * 128 : (ch + 1) * 128
                ]
        return 0

    for q in range(4):
        copies[q].wait()
        lax.fori_loop(q * 4, (q + 1) * 4, outer, 0)

    def convert(k, _):
        for j in range(16):
            rows = [tall[k * 8 + q, pl.ds(j * 11, 8, stride=3), :] for q in range(8)]
            xs[pl.ds(pl.multiple_of(k * 64, 64), 64), j * 128 : (j + 1) * 128] = (
                jnp.concatenate(rows, axis=0).astype(BF16)
            )
        return 0

    lax.fori_loop(0, 16, convert, 0)
    for copy in late:
        copy.wait()

    for j in range(0, 16, 2):
        part = dot(w[...], xs[:, j * 128 : (j + 2) * 128], TN)
        part = (part * (1.0 / 256) + bias).astype(BF16)
        for jj in range(2):
            for d in range(4):
                pair[lax.rem(d - depth + 4, 4), j + jj] = part[
                    d * 32 : (d + 1) * 32, jj * 128 : (jj + 1) * 128
                ]
    outs = []
    for m, ref in enumerate((p0_ref, p1_ref, p2_ref, p3_ref)):
        outs.append(pltpu.make_async_copy(pair.at[m], ref, sems.at[6 + m]))
        outs[-1].start()

    def weight(k, _):
        at = pl.multiple_of(k * 256, 256)
        gw[pl.ds(at, 256), :] = dot(xs[pl.ds(at, 256), :], st[...], NT).astype(BF16)
        return 0

    for half in range(2):
        lax.fori_loop(half * 2, half * 2 + 2, weight, 0)
        part = pl.ds(half * 512, 512)
        outs.append(pltpu.make_async_copy(gw.at[part], gw_ref.at[part], sems.at[10 + half]))
        outs[-1].start()
    for copy in outs:
        copy.wait()


def outer_call(lt, rt, st, w, bias):
    return pl.pallas_call(
        outer_kernel,
        out_shape=(
            *[jax.ShapeDtypeStruct((16, 32, 128), BF16)] * 4,
            jax.ShapeDtypeStruct((1024, 128), BF16),
        ),
        in_specs=(*hbm(1), *vmem(1), *hbm(2), *vmem(1)),
        out_specs=hbm(5),
        scratch_shapes=[
            pltpu.VMEM((128, 192, 128), F32),
            pltpu.VMEM((1024, 2048), BF16),
            pltpu.VMEM((4096, 256), BF16),
            pltpu.SemaphoreType.DMA((12,)),
            pltpu.VMEM((4, 16, 32, 128), BF16),
            pltpu.VMEM((128, 2048), BF16),
            pltpu.VMEM((1024, 128), BF16),
            pltpu.VMEM((1024, 128), BF16),
        ],
        cost_estimate=cost(11),
        name="outer",
    )(lt, rt, st, w, bias)


def back_kernel(
    gl_ref, gr_ref, normed_ref, wt_ref, count_ref, gw_ref,
    grad_ref, all_ref,
    sums, flat_ref,
):
    own = 16
    left = gl_ref[0].astype(F32)
    for k in range(1, 16):
        left = left + gl_ref[k].astype(F32)
    right = gr_ref[...].astype(F32)
    sums[0:256, :] = left.reshape(256, 128)
    sums[256:512, :] = right.reshape(256, 128)
    for i in range(own):
        t = [sums[pl.ds(side * 256 + i, 16, stride=own), :] for side in range(2)]
        grad_ref[:, i * 64 : (i + 1) * 64] = jnp.concatenate(
            [t[0][:, :64], t[0][:, 64:], t[1][:, :64], t[1][:, 64:]], axis=0
        ).astype(BF16)
    grad = grad_ref[...]
    both = dot(grad, normed_ref[...], NN)
    wt = wt_ref[...].astype(F32)
    column = jnp.sum(grad.astype(F32), axis=1, keepdims=True)
    gain = jnp.sum(both[:, 256:] * wt, axis=0, keepdims=True)
    shift = jnp.sum(column * wt, axis=0, keepdims=True)
    on = lax.broadcasted_iota(jnp.int32, (64, 128), 0) == lax.broadcasted_iota(
        jnp.int32, (64, 128), 1
    )
    bias = jnp.sum(jnp.where(on, column, 0.0), axis=0, keepdims=True)
    rows = [
        count_ref[...], gain[:, :128], gain[:, 128:], shift[:, :128], shift[:, 128:], bias,
    ]
    flat_ref[...] = jnp.zeros((16, 16, 128), F32)
    for k in range(8):
        flat_ref[k, 0:8, :] = both[k * 8 : (k + 1) * 8, :128]
        flat_ref[8 + k, 0:8, :] = both[k * 8 : (k + 1) * 8, 128:256]
    for k, row in enumerate(rows):
        hi = row.astype(BF16).astype(F32)
        flat_ref[k, 8:9, :] = hi
        flat_ref[k, 9:10, :] = row - hi
    for k in range(16):
        all_ref[k, 0:64, :] = gw_ref[k * 64 : (k + 1) * 64, :]
        all_ref[k, 64:80, :] = flat_ref[k].astype(BF16)


def back_call(gl, gr, normed, wt, count, gw):
    return pl.pallas_call(
        back_kernel,
        out_shape=(
            jax.ShapeDtypeStruct((64, 1024), BF16),
            jax.ShapeDtypeStruct((16, 80, 128), BF16),
        ),
        in_specs=vmem(6),
        out_specs=tuple(vmem(2)),
        scratch_shapes=[pltpu.VMEM((512, 128), F32), pltpu.VMEM((16, 16, 128), F32)],
        compiler_params=limit(8),
        cost_estimate=cost(2),
        name="back",
    )(gl, gr, normed, wt, count, gw)


def norm_kernel(
    x_ref, gain_ref, wt_ref, grad_ref, p0_ref, p1_ref, p2_ref, p3_ref,
    gx_ref, pair_ref,
    rows, rstds,
):
    seqs, own = 64, 16
    depth = lax.axis_index("depth")
    for m, ref in enumerate((p0_ref, p1_ref, p2_ref, p3_ref)):
        pair_ref[pl.ds(lax.rem(depth - m + 4, 4) * 16, 16)] = ref[...]
    gain = gain_ref[...]

    def block(k, _):
        x = x_ref[pl.ds(k * 128, 128), :].astype(F32)
        mean = jnp.mean(x, axis=-1, keepdims=True)
        centre = x - mean
        spread = jnp.mean(centre * centre, axis=-1, keepdims=True)
        rstd = lax.rsqrt(spread + EPSILON)
        y = centre * rstd
        rows[0, pl.ds(k * 128, 128), :] = y[:, :128]
        rows[1, pl.ds(k * 128, 128), :] = y[:, 128:]
        rstds[pl.ds(k * 128, 128), :] = jnp.broadcast_to(rstd, (128, 128))
        return 0

    lax.fori_loop(0, 8, block, 0)
    for i in range(own):
        gn = dot(grad_ref[:, i * seqs : (i + 1) * seqs], wt_ref[...], TN)
        hat = jnp.concatenate(
            [rows[h, pl.ds(i, seqs, stride=own), :] for h in range(2)], axis=1
        )
        rstd = rstds[pl.ds(i, seqs, stride=own), :][:, :1]
        g = gn * gain
        a = jnp.mean(g, axis=-1, keepdims=True)
        b = jnp.mean(g * hat, axis=-1, keepdims=True)
        gx = rstd * (g - a - hat * b)
        for h in range(2):
            rows[h, pl.ds(i, seqs, stride=own), :] = gx[:, h * 128 : (h + 1) * 128]
    for h in range(2):
        gx_ref[:, h * 128 : (h + 1) * 128] = rows[h].astype(BF16)


def norm_call(x, gain, wt, grad, pair):
    return pl.pallas_call(
        norm_kernel,
        out_shape=(
            jax.ShapeDtypeStruct((1024, 256), BF16),
            jax.ShapeDtypeStruct((64, 32, 128), BF16),
        ),
        in_specs=vmem(8),
        out_specs=tuple(vmem(2)),
        scratch_shapes=[pltpu.VMEM((2, 1024, 128), F32), pltpu.VMEM((1024, 128), F32)],
        compiler_params=limit(10),
        cost_estimate=cost(5),
        name="norm",
    )(x, gain, wt, grad, *pair)


def exchange(value, axis):
    return lax.all_to_all(value, axis, 0, 0, tiled=True)


def swap(value):
    return lax.ppermute(value, "col_1", [(0, 1), (1, 0)])


def place(d, r, c):
    return (d * 4 + r) * 8 + c


def right_pairs():
    return [
        (place(y, r, c), place(c % 4, y, 2 * r + c // 4))
        for y in range(4)
        for r in range(4)
        for c in range(8)
    ]


def rotate(value, axis, by):
    return lax.ppermute(value, axis, [(k, (k + by) % 4) for k in range(4)])


EVERY = ("depth", "row", "col_0", "col_1")
PLANE = ("depth", "row")


def summed(parts):
    return jnp.sum(parts.astype(F32), axis=0)


def give_kernel(a_ref, b_ref, out_ref):
    total = a_ref[...] + b_ref[...]
    row = total[72:73] + total[73:74]
    hi = row.astype(BF16).astype(F32)
    at = lax.broadcasted_iota(jnp.int32, (8, 128), 0)
    tail = jnp.where(at == 0, hi, jnp.where(at == 1, row - hi, 0.0))
    chunk = jnp.concatenate([total[:72], tail], axis=0).astype(BF16)
    for k in range(16):
        out_ref[k] = chunk


def give_call(a, b):
    return pl.pallas_call(
        give_kernel,
        out_shape=jax.ShapeDtypeStruct((16, 80, 128), BF16),
        in_specs=vmem(2),
        out_specs=vmem(1)[0],
        compiler_params=limit(2),
        cost_estimate=cost(1),
        name="give",
    )(a, b)


def finish_kernel(all_ref, gw_ref, pw_ref, pb_ref, ob_ref, gain_ref, shift_ref):
    for k in range(16):
        gw_ref[k * 64 : (k + 1) * 64, :] = all_ref[k, 0:64, :].astype(F32)
    rows = []
    for k in range(8):
        for half in range(2):
            pw_ref[k * 8 : (k + 1) * 8, half * 128 : (half + 1) * 128] = all_ref[
                half * 8 + k, 64:72, :
            ].astype(F32)
        tail = all_ref[k, 72:80, :].astype(F32)
        rows.append(tail[0:1] + tail[1:2])
    ob_ref[...] = rows[0]
    gain_ref[...] = jnp.concatenate(rows[1:3], axis=1)
    shift_ref[...] = jnp.concatenate(rows[3:5], axis=1)
    pb_ref[...] = rows[5][:, :64]


def finish_call(total):
    return pl.pallas_call(
        finish_kernel,
        out_shape=(
            jax.ShapeDtypeStruct((1024, 128), F32),
            jax.ShapeDtypeStruct((64, 256), F32),
            jax.ShapeDtypeStruct((1, 64), F32),
            jax.ShapeDtypeStruct((1, 128), F32),
            jax.ShapeDtypeStruct((1, 256), F32),
            jax.ShapeDtypeStruct((1, 256), F32),
        ),
        in_specs=vmem(1),
        out_specs=tuple(vmem(6)),
        compiler_params=limit(4),
        cost_estimate=cost(1),
        name="finish",
    )(total)


def step(
    alignment, norm_gain, norm_shift, proj_weight, proj_bias, out_weight, out_bias, cotangent
):
    x = alignment.reshape(1024, 256)
    gain = norm_gain.reshape(1, 256)
    shift = norm_shift.reshape(1, 256)
    wt = proj_weight.T
    cot = exchange(jnp.transpose(cotangent, (1, 2, 0)).reshape(4, 16, 32, 128), "depth")
    left, right, normed = sides_call(x, gain, shift, wt, proj_bias.reshape(1, 64))
    pairs = right_pairs()
    near = exchange(left, ("depth", "col_0"))
    rights = [lax.ppermute(right, EVERY, pairs)]
    for m in range(1, 4):
        rights.append(rotate(rights[0], "row", m))
    far = swap(near)

    gp, st, count = grad_call(cot, out_weight)
    keep, send, rt = left_call(rights, gp)
    came = swap(send)
    mine = (keep.astype(F32) + came.astype(F32)).astype(BF16)
    lefts = exchange(mine, ("depth", "col_0"))

    *gr, lt = right_call(near, far, gp)
    for m in range(1, 4):
        gr[m] = rotate(gr[m], "row", m)
    right_grad = sum(g.astype(F32) for g in gr).astype(BF16)
    right_grad = lax.ppermute(right_grad, EVERY, [(b, a) for a, b in pairs])

    *pair, gw = outer_call(lt, rt, st, out_weight, out_bias.reshape(1, 128))
    grad, total = back_call(lefts, right_grad, normed, wt, count, gw)

    total = exchange(total, PLANE)
    total = summed(total)
    for m in (1, 3):
        total = total + lax.ppermute(total, "col_0", [(k, k ^ m) for k in range(4)])
    other = swap(total)
    total = give_call(total, other)
    total = exchange(total, PLANE)
    for m in range(1, 4):
        pair[m] = rotate(pair[m], "depth", m)
    gx, pair = norm_call(x, gain, wt, grad, pair)
    gw, gpw, gpb, gb, gg, gs = finish_call(total)
    return (
        jnp.transpose(pair, (2, 0, 1)),
        gx.reshape(alignment.shape),
        gpw.T,
        gpb.reshape(64),
        gw,
        gb.reshape(128),
        gg.reshape(256),
        gs.reshape(256),
    )


def solution(mesh):
    split = Mesh(mesh.devices.reshape(4, 4, 4, 2), EVERY)
    side = P("depth", ("row", "col_0", "col_1"), None)
    block = P("row", ("col_0", "col_1"), "depth")
    return jax.shard_map(
        step,
        mesh=split,
        in_specs=(side, P(), P(), P(), P(), P(), P(), block),
        out_specs=(block, side, P(), P(), P(), P(), P(), P()),
        check_vma=False,
    )
```
